128 devices in a mesh: batch: 1, head: 2 (over core), seq: 64 (over z, y, x).
Axes of the slice: x: 4, y: 4, z: 4, core: 2. Of those that a mesh axis runs over, the one named last changes fastest.
Arguments:
- x_embed: bfloat16 [16384, 2048], P(('batch', 'seq'))
- positions: int32 [16384], P(('batch', 'seq'))
- w_q: bfloat16 [2, 2048, 32, 64], P(None, None, 'head')
- w_k: bfloat16 [2, 2048, 8, 64], P(None, None, 'head')
- w_v: bfloat16 [2, 2048, 8, 64], P(None, None, 'head')
- w_o: bfloat16 [2, 32, 64, 2048], P(None, 'head')
- w_gate: bfloat16 [2, 2048, 8192], P(None, None, 'head')
- w_up: bfloat16 [2, 2048, 8192], P(None, None, 'head')
- w_down: bfloat16 [2, 8192, 2048], P(None, 'head')
- norm_gain: bfloat16 [2, 2048], replicated
Outputs:
- output 1: bfloat16 [16384, 2048], P(('batch', 'seq'))
- output 2: bfloat16 [2, 16384, 8, 64], P(None, ('batch', 'seq'), 'head')
- output 3: bfloat16 [2, 16384, 8, 64], P(None, ('batch', 'seq'), 'head')
All inputs are finite; a program needn't handle non-finite values.
Results may differ from the reference program's by a relative error of at most 0.02.
Values are sent between devices in bfloat16 or wider.
A program may use at most 1 GiB of HBM per device.

```python
import math
import jax
import jax.numpy as jnp
from jax import lax

SEQ_LEN = 16384
D_MODEL = 2048
NUM_HEADS = 32
KV_HEADS = 8
HEAD_DIM = 64
FF_DIM = 8192
LAYERS = 2
QUERY_BLOCK = 128
ROPE_BASE = 500000
EPS = 1e-5


def draw_normal(rng_key, arr_shape, std_scale):
    return (jax.random.normal(rng_key, arr_shape, jnp.float32) * std_scale).astype(jnp.bfloat16)


def setup_inputs(seed: int = 0, part: int = 0) -> dict:
    shared_root, part_root = jax.random.split(jax.random.key(seed))
    part_key = jax.random.fold_in(part_root, part)
    key_embed, key_gap, key_offset = jax.random.split(part_key, 3)
    weight_keys = jax.random.split(shared_root, 8)
    logit_std = math.sqrt(0.5 * math.log(SEQ_LEN))
    qk_scale = math.sqrt(logit_std / D_MODEL)
    out_scale = 0.5 * SEQ_LEN ** 0.25 / math.sqrt(NUM_HEADS * HEAD_DIM)
    x_embed = draw_normal(key_embed, (SEQ_LEN, D_MODEL), 1.0)
    pos_gaps = jax.random.randint(key_gap, (SEQ_LEN,), 1, 4)
    offset = jax.random.randint(key_offset, (), 0, 1024)
    positions = (offset + jnp.cumsum(pos_gaps) - pos_gaps[0]).astype(jnp.int32)
    gains = 1.0 + 0.3 * jax.random.normal(weight_keys[7], (LAYERS, D_MODEL), jnp.float32)
    return {
        'x_embed': x_embed,
        'positions': positions,
        'w_q': draw_normal(weight_keys[0], (LAYERS, D_MODEL, NUM_HEADS, HEAD_DIM), qk_scale),
        'w_k': draw_normal(weight_keys[1], (LAYERS, D_MODEL, KV_HEADS, HEAD_DIM), qk_scale),
        'w_v': draw_normal(weight_keys[2], (LAYERS, D_MODEL, KV_HEADS, HEAD_DIM), D_MODEL ** -0.5),
        'w_o': draw_normal(weight_keys[3], (LAYERS, NUM_HEADS, HEAD_DIM, D_MODEL), out_scale),
        'w_gate': draw_normal(weight_keys[4], (LAYERS, D_MODEL, FF_DIM), D_MODEL ** -0.5),
        'w_up': draw_normal(weight_keys[5], (LAYERS, D_MODEL, FF_DIM), D_MODEL ** -0.5),
        'w_down': draw_normal(weight_keys[6], (LAYERS, FF_DIM, D_MODEL), 1.5 * FF_DIM ** -0.5),
        'norm_gain': gains.astype(jnp.bfloat16),
    }


def rms_norm(x_in, gain_row):
    x_f32 = x_in.astype(jnp.float32)
    inv_rms = lax.rsqrt(jnp.mean(x_f32 * x_f32, axis=-1, keepdims=True) + EPS)
    return (x_f32 * inv_rms * gain_row.astype(jnp.float32)).astype(jnp.bfloat16)


def rope_tables(positions):
    half_dim = HEAD_DIM // 2
    inv_freq = float(ROPE_BASE) ** (-(jnp.arange(half_dim, dtype=jnp.float32) * 2.0 / HEAD_DIM))
    angles = positions.astype(jnp.float32)[..., None] * inv_freq
    return jnp.cos(angles), jnp.sin(angles)


def apply_rope(heads_in, cos_t, sin_t):
    half_dim = heads_in.shape[-1] // 2
    heads_f32 = heads_in.astype(jnp.float32)
    first_half = heads_f32[..., :half_dim]
    second_half = heads_f32[..., half_dim:]
    cos_b = cos_t[..., None, :]
    sin_b = sin_t[..., None, :]
    rotated = jnp.concatenate([first_half * cos_b - second_half * sin_b, second_half * cos_b + first_half * sin_b], axis=-1)
    return rotated.astype(jnp.bfloat16)


def causal_attention(q_rot, k_rot, v_heads):
    group_size = NUM_HEADS // KV_HEADS
    logit_scale = 1.0 / math.sqrt(HEAD_DIM)
    num_blocks = SEQ_LEN // QUERY_BLOCK
    q_blocks = q_rot.reshape(num_blocks, QUERY_BLOCK, KV_HEADS, group_size, HEAD_DIM).astype(jnp.float32)
    k_f32 = k_rot.astype(jnp.float32)
    v_f32 = v_heads.astype(jnp.float32)
    key_index = jnp.arange(SEQ_LEN)

    def one_block(block_args):
        block_id, q_blk = block_args
        logits = jnp.einsum('qkgd,skd->qkgs', q_blk, k_f32) * logit_scale
        query_index = block_id * QUERY_BLOCK + jnp.arange(QUERY_BLOCK)
        allowed = (query_index[:, None] >= key_index[None, :])[:, None, None, :]
        logits = jnp.where(allowed, logits, -jnp.inf)
        row_max = jnp.max(logits, axis=-1, keepdims=True)
        prob_f32 = jnp.exp(logits - row_max)
        row_sum = jnp.sum(prob_f32, axis=-1, keepdims=True)
        prob_low = prob_f32.astype(jnp.bfloat16).astype(jnp.float32)
        return jnp.einsum('qkgs,skd->qkgd', prob_low, v_f32) / row_sum

    block_out = lax.map(one_block, (jnp.arange(num_blocks), q_blocks))
    return block_out.reshape(SEQ_LEN, NUM_HEADS * HEAD_DIM).astype(jnp.bfloat16)


def reference(x_embed, positions, w_q, w_k, w_v, w_o, w_gate, w_up, w_down, norm_gain):
    cos_t, sin_t = rope_tables(positions)

    def layer_step(x_cur, layer_weights):
        wq_l, wk_l, wv_l, wo_l, wg_l, wu_l, wd_l, gain_row = layer_weights
        normed = rms_norm(x_cur, gain_row)
        q_proj = jnp.dot(normed, wq_l.reshape(D_MODEL, NUM_HEADS * HEAD_DIM), preferred_element_type=jnp.float32).astype(jnp.bfloat16)
        k_proj = jnp.dot(normed, wk_l.reshape(D_MODEL, KV_HEADS * HEAD_DIM), preferred_element_type=jnp.float32).astype(jnp.bfloat16)
        v_proj = jnp.dot(normed, wv_l.reshape(D_MODEL, KV_HEADS * HEAD_DIM), preferred_element_type=jnp.float32).astype(jnp.bfloat16)
        q_rot = apply_rope(q_proj.reshape(SEQ_LEN, NUM_HEADS, HEAD_DIM), cos_t, sin_t)
        k_rot = apply_rope(k_proj.reshape(SEQ_LEN, KV_HEADS, HEAD_DIM), cos_t, sin_t)
        v_heads = v_proj.reshape(SEQ_LEN, KV_HEADS, HEAD_DIM)
        attn_heads = causal_attention(q_rot, k_rot, v_heads)
        attn_part = jnp.dot(attn_heads, wo_l.reshape(NUM_HEADS * HEAD_DIM, D_MODEL), preferred_element_type=jnp.float32)
        gate_f32 = jnp.dot(normed, wg_l, preferred_element_type=jnp.float32)
        up_f32 = jnp.dot(normed, wu_l, preferred_element_type=jnp.float32)
        hidden = (jax.nn.silu(gate_f32) * up_f32).astype(jnp.bfloat16)
        mlp_part = jnp.dot(hidden, wd_l, preferred_element_type=jnp.float32)
        update = (attn_part + mlp_part).astype(jnp.bfloat16)
        x_next = (x_cur.astype(jnp.float32) + update.astype(jnp.float32)).astype(jnp.bfloat16)
        return x_next, (k_rot, v_heads)

    stacked = (w_q, w_k, w_v, w_o, w_gate, w_up, w_down, norm_gain)
    x_out, caches = lax.scan(layer_step, x_embed, stacked)
    return x_out, caches[0], caches[1]
```

```python
import functools
import jax
import jax.numpy as jnp
from jax import lax
from jax.experimental import pallas as pl
from jax.experimental.pallas import tpu as pltpu
from jax.sharding import PartitionSpec as P

ROPE_BASE = 500000.0
EPS = 1e-5
LOG2E = 1.4426950408889634
NEG = -1e30
MESH = pl.DeviceIdType.MESH
F32 = jnp.float32
BF16 = jnp.bfloat16
VMEM_LIMIT = 62 * 1024 * 1024

DIM_ORDER = (((0, 1, 2), (0, 1, 2), (1, 2, 0), (2, 0, 1)), ((0, 1, 2), (1, 2, 0), (1, 2, 0), (2, 0, 1)))


def rope_tables(positions, head_dim):
    half_dim = head_dim // 2
    inv_freq = ROPE_BASE ** (-(jnp.arange(half_dim, dtype=F32) * 2.0 / head_dim))
    angles = positions.astype(F32)[..., None] * inv_freq
    return jnp.cos(angles), jnp.sin(angles)


class Place:
    def __init__(self):
        self.seq = lax.axis_index('seq')
        self.head = lax.axis_index('head')
        self.xyz = (self.seq % 4, (self.seq // 4) % 4, self.seq // 16)
        self.mem = tuple(c // 2 for c in self.xyz)
        self.cls = tuple(((c + 1) // 2) % 2 for c in self.xyz)
        self.core = (self.mem[0] + self.mem[1]) % 2
        self.kv_local = 2 * self.mem[1] + self.mem[0]
        self.member = 2 * self.mem[2] + self.mem[0]

    def is_self(self):
        same_z = 1 - lax.rem(self.head + self.mem[2], 2)
        same_c = 1 - lax.rem(self.head + self.core, 2)
        return same_z * same_c

    def at(self, mem, cls):
        cs = [m * 3 + c * (1 - 2 * m) for m, c in zip(mem, cls)]
        return cs[2] * 16 + cs[1] * 4 + cs[0]

    def target(self, t):
        return self.at((t % 2, t // 2, self.head), self.cls)

    def source_mem(self, i):
        mx, mz = i % 2, i // 2
        return (mx, (mx + self.head) % 2, mz)

    def source(self, i, flips=()):
        cls = [1 - c if d in flips else c for d, c in enumerate(self.cls)]
        return self.at(self.source_mem(i), cls)

    def partner(self, dim):
        cls = [1 - c if d == dim else c for d, c in enumerate(self.cls)]
        return self.at(self.mem, cls)

    def dev(self, seq, head):
        return {'seq': seq, 'head': head}


def rope_lanes(x, cos, sin):
    lane = lax.broadcasted_iota(jnp.int32, (x.shape[0], 128), 1)
    first = (lane % 64) < 32
    out = []
    for c in range(x.shape[1] // 128):
        part = x[:, c * 128:(c + 1) * 128]
        rot = jnp.where(first, pltpu.roll(part, 96, 1), pltpu.roll(part, 32, 1))
        out.append((part * cos + rot * sin).astype(BF16))
    return jnp.concatenate(out, axis=1)


def front_kernel(layer, x_ref, gain_ref, cos_ref, sin_ref, cosT_ref, sinT_ref, wq, wk, wv, wg, wu, wd, kT_ref, vT_ref, q_all, kv_all, mlp_ref, h_ref, q_send, kv_send, wqb, wkb, wvb, wgb, wub, wdb, wsem, msem, skv, sq, sag, sdd, rkv, rq, rag, rdd):
    me = Place()
    sib = 1 - me.head
    n_tiles = 16
    flag = me.is_self()

    barrier = pltpu.get_barrier_semaphore()
    for i in range(4):
        mem = me.source_mem(i)
        src_self = flag * (1 - lax.rem(i // 2 + me.mem[2], 2)) * (1 - lax.rem(i % 2 + me.mem[0], 2))

        @pl.when(src_self == 0)
        def _():
            pl.semaphore_signal(barrier, inc=1, device_id=me.dev(me.source(i), me.mem[2]), device_id_type=MESH)
    for d in range(3):
        pl.semaphore_signal(barrier, inc=1, device_id=me.dev(me.partner(d), me.head), device_id_type=MESH)
    pl.semaphore_signal(barrier, inc=1, device_id=me.dev(me.seq, sib), device_id_type=MESH)

    cps = [pltpu.make_async_copy(wk.at[layer], wkb, wsem.at[0]), pltpu.make_async_copy(wv.at[layer], wvb, wsem.at[1])]
    for t in range(4):
        cps.append(pltpu.make_async_copy(wq.at[layer, pl.ds(t * 256, 256)], wqb.at[t], wsem.at[2 + t]))
    for c in cps:
        c.start()

    def tile_copies(n, slot):
        return (pltpu.make_async_copy(wg.at[layer, :, pl.ds(pl.multiple_of(n * 256, 256), 256)], wgb.at[slot], msem.at[slot, 0]),
                pltpu.make_async_copy(wu.at[layer, :, pl.ds(pl.multiple_of(n * 256, 256), 256)], wub.at[slot], msem.at[slot, 1]),
                pltpu.make_async_copy(wd.at[layer, pl.ds(pl.multiple_of(n * 256, 256), 256)], wdb.at[slot], msem.at[slot, 2]))

    for n in range(3):
        for c in tile_copies(n, n):
            c.start()

    xf = x_ref[...].astype(F32)
    inv = lax.rsqrt(jnp.mean(xf * xf, axis=-1, keepdims=True) + EPS)
    h_ref[...] = (xf * inv * gain_ref[layer:layer + 1, :].astype(F32)).astype(BF16)

    nt = (((1,), (1,)), ((), ()))
    cps[0].wait()
    kT = lax.dot_general(wkb[...], h_ref[...], nt, preferred_element_type=F32).astype(BF16).astype(F32)
    cosT, sinT = cosT_ref[...], sinT_ref[...]
    for t in range(4):
        a, b = kT[t * 64:t * 64 + 32], kT[t * 64 + 32:t * 64 + 64]
        ra, rb = (a * cosT - b * sinT).astype(BF16), (b * cosT + a * sinT).astype(BF16)
        kv_send[t, 0:32, :] = ra
        kv_send[t, 32:64, :] = rb
        kT_ref[t * 64:t * 64 + 32, :] = ra
        kT_ref[t * 64 + 32:t * 64 + 64, :] = rb
    cps[1].wait()
    vT = lax.dot_general(wvb[...], h_ref[...], nt, preferred_element_type=F32).astype(BF16)
    vT_ref[...] = vT
    for t in range(4):
        kv_send[t, 64:128, :] = vT[t * 64:(t + 1) * 64]

    pl.semaphore_wait(barrier, 8 - flag)

    def kv_copy(t):
        return pltpu.make_async_remote_copy(src_ref=kv_send.at[t], dst_ref=kv_all.at[me.seq], send_sem=skv.at[t], recv_sem=rkv.at[me.member], device_id=me.dev(me.target(t), me.core), device_id_type=MESH)

    def q_copy(t):
        return pltpu.make_async_remote_copy(src_ref=q_send.at[t], dst_ref=q_all.at[me.member], send_sem=sq.at[t], recv_sem=rq.at[me.member], device_id=me.dev(me.target(t), me.core), device_id_type=MESH)

    def t_self(t):
        return flag * (1 - lax.rem(t // 2 + me.mem[1], 2)) * (1 - lax.rem(t % 2 + me.mem[0], 2))

    def send_all(make, src, dst, idx):
        for t in range(4):
            @pl.when(t_self(t) == 0)
            def _():
                make(t).start()

            @pl.when(t_self(t) == 1)
            def _():
                dst[idx] = src[t]

    send_all(kv_copy, kv_send, kv_all, me.seq)

    cos, sin = cos_ref[...], sin_ref[...]
    for t in range(4):
        cps[2 + t].wait()
        q = lax.dot_general(h_ref[...], wqb[t], nt, preferred_element_type=F32).astype(BF16).astype(F32)
        q_send[t] = rope_lanes(q, cos, sin)
    send_all(q_copy, q_send, q_all, me.member)

    def ag_plan(i):
        plans = []
        for core in range(2):
            d1, d2, d3 = DIM_ORDER[core][i]
            plans.append([(d1, ()), (d2, ()), (d2, (d1,)), (d3, ()), (d3, (d1,)), (d3, (d2,)), (d3, (d1, d2))])
        return plans

    def ag_copy(core, i, k):
        dim, flips = ag_plan(i)[core][k]
        pos = me.source(i, flips)
        return pltpu.make_async_remote_copy(src_ref=kv_all.at[pos], dst_ref=kv_all.at[pos], send_sem=sag.at[i, k], recv_sem=rag.at[i, k], device_id=me.dev(me.partner(dim), me.head), device_id_type=MESH)

    def got_flips(core, i, k):
        dim, flips = ag_plan(i)[core][k]
        return tuple(flips) + (dim,)

    def ag_recv(core, i, k):
        pos = me.source(i, got_flips(core, i, k))
        pltpu.make_async_remote_copy(src_ref=kv_all.at[pos], dst_ref=kv_all.at[pos], send_sem=sag.at[i, k], recv_sem=rag.at[i, k], device_id=me.dev(me.seq, sib), device_id_type=MESH).wait_recv()

    def dd_copy(pos, i, k):
        return pltpu.make_async_remote_copy(src_ref=kv_all.at[pos], dst_ref=kv_all.at[pos], send_sem=sdd.at[i, k], recv_sem=rdd.at[i, k], device_id=me.dev(me.seq, sib), device_id_type=MESH)

    def s_self(i):
        return flag * (1 - lax.rem(i // 2 + me.mem[2], 2)) * (1 - lax.rem(i % 2 + me.mem[0], 2))

    def per_core(fn):
        for core in range(2):
            @pl.when(me.head == core)
            def _():
                fn(core)

    def phase1(core):
        for i in range(4):
            @pl.when(s_self(i) == 0)
            def _():
                pltpu.make_async_remote_copy(src_ref=kv_send.at[0], dst_ref=kv_all.at[me.source(i)], send_sem=skv.at[0], recv_sem=rkv.at[i], device_id=me.dev(me.seq, sib), device_id_type=MESH).wait_recv()
            ag_copy(core, i, 0).start()
        for k in (1, 3):
            for i in range(4):
                ag_copy(core, i, k).start()
        for i in range(4):
            dd_copy(me.source(i), i, 0).start()

    def phase2(core):
        for i in range(4):
            ag_recv(core, i, 0)
            ag_copy(core, i, 2).start()
            ag_copy(core, i, 4).start()
            dd_copy(me.source(i, got_flips(core, i, 0)), i, 1).start()
        for i in range(4):
            ag_recv(core, i, 1)
            ag_copy(core, i, 5).start()
            dd_copy(me.source(i, got_flips(core, i, 1)), i, 2).start()

    def phase3(core):
        for i in range(4):
            ag_recv(core, i, 2)
            ag_copy(core, i, 6).start()
            dd_copy(me.source(i, got_flips(core, i, 2)), i, 3).start()

    def phase4(core):
        for k in range(3, 7):
            for i in range(4):
                ag_recv(core, i, k)
                dd_copy(me.source(i, got_flips(core, i, k)), i, k + 1).start()

    def phase5(core):
        other = 1 - core
        for k in range(8):
            for i in range(4):
                mx, mz = i % 2, i // 2
                mem = (mx, (mx + other) % 2, mz)
                flips = () if k == 0 else got_flips(other, i, k - 1)
                cls = [1 - c if d in flips else c for d, c in enumerate(me.cls)]
                dd_copy(me.at(mem, cls), i, k).wait_recv()
        for i in range(4):
            for k in range(7):
                ag_copy(core, i, k).wait_send()
            for k in range(8):
                dd_copy(me.source(i), i, k).wait_send()

    mlp_ref[...] = jnp.zeros_like(mlp_ref)

    def tile(n, carry):
        slot = n % 3
        for c in tile_copies(n, slot):
            c.wait()
        for at, fn in ((4, phase1), (9, phase2), (13, phase3)):
            @pl.when(n == at)
            def _():
                per_core(fn)
        g = jnp.dot(h_ref[...], wgb[slot], preferred_element_type=F32)
        u = jnp.dot(h_ref[...], wub[slot], preferred_element_type=F32)
        hid = (g * jax.nn.sigmoid(g) * u).astype(BF16)
        mlp_ref[...] += jnp.dot(hid, wdb[slot], preferred_element_type=F32)

        @pl.when(n + 3 < n_tiles)
        def _():
            for c in tile_copies(n + 3, slot):
                c.start()
        return carry

    lax.fori_loop(0, n_tiles, tile, 0)
    per_core(phase4)
    per_core(phase5)
    for t in range(4):
        @pl.when(t_self(t) == 0)
        def _():
            kv_copy(t).wait_send()
            q_copy(t).wait_send()
    for i in range(4):
        @pl.when(s_self(i) == 0)
        def _():
            pltpu.make_async_remote_copy(src_ref=q_send.at[0], dst_ref=q_all.at[i], send_sem=sq.at[0], recv_sem=rq.at[i], device_id=me.dev(me.seq, sib), device_id_type=MESH).wait_recv()


def attn_tile(q, kT, vT, m_ref, l_ref, acc_ref, rows, mask=None):
    s = jnp.dot(q, kT, preferred_element_type=F32) * (LOG2E / 8.0)
    if mask is not None:
        s = jnp.where(mask, s, NEG)
    m_old = m_ref[rows, :]
    m_new = jnp.maximum(m_old, jnp.broadcast_to(jnp.max(s, axis=1, keepdims=True), m_old.shape))
    alpha = jnp.exp2(m_old - m_new)
    lsum = l_ref[rows, :] * alpha
    ps = []
    for c in range(s.shape[1] // 128):
        p = jnp.exp2(s[:, c * 128:(c + 1) * 128] - m_new)
        lsum = lsum + p
        ps.append(p.astype(BF16))
    l_ref[rows, :] = lsum
    pv = lax.dot_general(jnp.concatenate(ps, axis=1), vT, (((1,), (1,)), ((), ())), preferred_element_type=F32)
    acc_ref[rows, :] = acc_ref[rows, :] * alpha[:, :64] + pv
    m_ref[rows, :] = m_new


def attn_kernel(q_ref, kv_ref, o_ref, qp, m_ref, l_ref, acc_ref):
    me = Place()
    nb, mc = 4, 512

    def block(i, carry):
        pos = me.source(i)
        qb = q_ref[i]
        for g in range(4):
            qp[pl.ds(g * 256, 256), :] = qb[:, g * 64:(g + 1) * 64]
        m_ref[...] = jnp.full_like(m_ref, NEG)
        l_ref[...] = jnp.zeros_like(l_ref)
        acc_ref[...] = jnp.zeros_like(acc_ref)

        def wide(n, c):
            kT = jnp.concatenate([kv_ref[n * nb + b, :64, :] for b in range(nb)], axis=1)
            vT = jnp.concatenate([kv_ref[n * nb + b, 64:, :] for b in range(nb)], axis=1)
            for r in range(1024 // mc):
                rows = pl.ds(r * mc, mc)
                attn_tile(qp[rows, :], kT, vT, m_ref, l_ref, acc_ref, rows)
            return c

        lax.fori_loop(0, pos // nb, wide, 0)

        def narrow(n, c):
            for r in range(1024 // mc):
                rows = pl.ds(r * mc, mc)
                attn_tile(qp[rows, :], kv_ref[n, :64, :], kv_ref[n, 64:, :], m_ref, l_ref, acc_ref, rows)
            return c

        lax.fori_loop((pos // nb) * nb, pos, narrow, 0)
        ri = lax.broadcasted_iota(jnp.int32, (256, 256), 0)
        ci = lax.broadcasted_iota(jnp.int32, (256, 256), 1)
        for g in range(4):
            rows = pl.ds(g * 256, 256)
            attn_tile(qp[rows, :], kv_ref[pos, :64, :], kv_ref[pos, 64:, :], m_ref, l_ref, acc_ref, rows, ri >= ci)
        outs = []
        for g in range(4):
            rows = pl.ds(g * 256, 256)
            l = jnp.sum(l_ref[rows, :], axis=1, keepdims=True)
            outs.append((acc_ref[rows, :] / l).astype(BF16))
        o_ref[i] = jnp.concatenate(outs, axis=1)
        return carry

    lax.fori_loop(0, 4, block, 0)


def back_kernel(layer, o_ref, mlp_ref, x_ref, wo, out_ref, o_full, part, part_in, wob, wsem, so, ro, sp, rp):
    me = Place()
    sib = 1 - me.head
    flag = me.is_self()
    barrier = pltpu.get_barrier_semaphore()

    def s_self(i):
        return flag * (1 - lax.rem(i // 2 + me.mem[2], 2)) * (1 - lax.rem(i % 2 + me.mem[0], 2))

    def t_self(t):
        return flag * (1 - lax.rem(t // 2 + me.mem[1], 2)) * (1 - lax.rem(t % 2 + me.mem[0], 2))

    for t in range(4):
        @pl.when(t_self(t) == 0)
        def _():
            pl.semaphore_signal(barrier, inc=1, device_id=me.dev(me.target(t), me.core), device_id_type=MESH)
    pl.semaphore_signal(barrier, inc=1, device_id=me.dev(me.seq, sib), device_id_type=MESH)
    wcps = [pltpu.make_async_copy(wo.at[layer, pl.ds(t * 256, 256)], wob.at[t], wsem.at[t]) for t in range(4)]
    for c in wcps:
        c.start()
    pl.semaphore_wait(barrier, 5 - flag)

    def o_copy(i):
        return pltpu.make_async_remote_copy(src_ref=o_ref.at[i], dst_ref=o_full.at[me.kv_local], send_sem=so.at[i], recv_sem=ro.at[me.kv_local], device_id=me.dev(me.source(i), me.mem[2]), device_id_type=MESH)

    for i in range(4):
        @pl.when(s_self(i) == 0)
        def _():
            o_copy(i).start()

        @pl.when(s_self(i) == 1)
        def _():
            o_full[me.kv_local] = o_ref[i]
    for t in range(4):
        wcps[t].wait()
    for t in range(4):
        @pl.when(t_self(t) == 0)
        def _():
            pltpu.make_async_remote_copy(src_ref=o_ref.at[0], dst_ref=o_full.at[t], send_sem=so.at[0], recv_sem=ro.at[t], device_id=me.dev(me.seq, sib), device_id_type=MESH).wait_recv()

    def p_copy(n):
        return pltpu.make_async_remote_copy(src_ref=part.at[n], dst_ref=part_in.at[n], send_sem=sp.at[n], recv_sem=rp.at[n], device_id=me.dev(me.seq, sib), device_id_type=MESH)

    for n in range(8):
        cols = pl.ds(n * 256, 256)
        acc = mlp_ref[:, cols]
        for t in range(4):
            acc = acc + jnp.dot(o_full[t], wob[t, :, cols], preferred_element_type=F32)
        part[n] = acc
        p_copy(n).start()
    for n in range(8):
        cols = pl.ds(n * 256, 256)
        p_copy(n).wait_recv()
        y = (part[n] + part_in[n]).astype(BF16)
        out_ref[:, cols] = (x_ref[:, cols].astype(F32) + y.astype(F32)).astype(BF16)
    for n in range(8):
        p_copy(n).wait_send()
    for i in range(4):
        @pl.when(s_self(i) == 0)
        def _():
            o_copy(i).wait_send()


def vm():
    return pl.BlockSpec(memory_space=pltpu.VMEM)


def hbm():
    return pl.BlockSpec(memory_space=pl.ANY)


def sds(shape, dtype):
    return jax.ShapeDtypeStruct(shape, dtype)


def dma(*shape):
    return pltpu.SemaphoreType.DMA(shape)


def solution(mesh):
    row_spec = P(('batch', 'seq'), None)
    pos_spec = P(('batch', 'seq'))
    head_spec = P(None, None, 'head', None)
    out_proj_spec = P(None, 'head', None, None)
    col_spec = P(None, None, 'head')
    down_spec = P(None, 'head', None)
    cache_spec = P(None, ('batch', 'seq'), 'head', None)

    def local_forward(x, pos, w_q, w_k, w_v, w_o, w_gate, w_up, w_down, gain):
        cos, sin = rope_tables(pos, 64)
        cos_l = jnp.concatenate([cos] * 4, axis=1)
        sin_l = jnp.concatenate([-sin, sin, -sin, sin], axis=1)
        cosT, sinT = cos.T, sin.T
        wq = w_q.transpose(0, 2, 3, 1).reshape(2, 1024, 2048)
        wk = w_k.transpose(0, 2, 3, 1).reshape(2, 256, 2048)
        wv = w_v.transpose(0, 2, 3, 1).reshape(2, 256, 2048)
        wo = w_o.reshape(2, 1024, 2048)
        ks, vs = [], []
        for layer in range(2):
            kT, vT, q_all, kv_all, mlp = pl.pallas_call(
                functools.partial(front_kernel, layer),
                out_shape=(sds((256, 256), BF16), sds((256, 256), BF16), sds((4, 256, 256), BF16), sds((64, 128, 256), BF16), sds((256, 2048), F32)),
                in_specs=[vm()] * 6 + [hbm()] * 6,
                out_specs=[vm()] * 5,
                scratch_shapes=[
                    pltpu.VMEM((256, 2048), BF16), pltpu.VMEM((4, 256, 256), BF16), pltpu.VMEM((4, 128, 256), BF16),
                    pltpu.VMEM((4, 256, 2048), BF16), pltpu.VMEM((256, 2048), BF16), pltpu.VMEM((256, 2048), BF16),
                    pltpu.VMEM((3, 2048, 256), BF16), pltpu.VMEM((3, 2048, 256), BF16), pltpu.VMEM((3, 256, 2048), BF16),
                    dma(6), dma(3, 3), dma(4), dma(4), dma(4, 7), dma(4, 8), dma(4), dma(4), dma(4, 7), dma(4, 8)],
                compiler_params=pltpu.CompilerParams(collective_id=2 * layer, has_side_effects=True, vmem_limit_bytes=VMEM_LIMIT),
                name=f'front{layer}',
            )(x, gain, cos_l, sin_l, cosT, sinT, wq, wk, wv, w_gate, w_up, w_down)
            o = pl.pallas_call(
                attn_kernel,
                out_shape=sds((4, 256, 256), BF16),
                in_specs=[vm()] * 2,
                out_specs=vm(),
                scratch_shapes=[pltpu.VMEM((1024, 64), BF16), pltpu.VMEM((1024, 128), F32), pltpu.VMEM((1024, 128), F32), pltpu.VMEM((1024, 64), F32)],
                compiler_params=pltpu.CompilerParams(vmem_limit_bytes=VMEM_LIMIT),
                name='attn',
            )(q_all, kv_all)
            x = pl.pallas_call(
                functools.partial(back_kernel, layer),
                out_shape=sds((256, 2048), BF16),
                in_specs=[vm()] * 3 + [hbm()],
                out_specs=vm(),
                scratch_shapes=[pltpu.VMEM((4, 256, 256), BF16), pltpu.VMEM((8, 256, 256), F32), pltpu.VMEM((8, 256, 256), F32), pltpu.VMEM((4, 256, 2048), BF16),
                                dma(4), dma(4), dma(4), dma(8), dma(8)],
                compiler_params=pltpu.CompilerParams(collective_id=2 * layer + 1, has_side_effects=True, vmem_limit_bytes=VMEM_LIMIT),
                name=f'back{layer}',
            )(o, mlp, x, wo)
            ks.append(kT)
            vs.append(vT)
        k_cache = jnp.stack(ks).reshape(2, 4, 64, 256).transpose(0, 3, 1, 2)
        v_cache = jnp.stack(vs).reshape(2, 4, 64, 256).transpose(0, 3, 1, 2)
        return x, k_cache, v_cache

    return jax.shard_map(local_forward, mesh=mesh, in_specs=(row_spec, pos_spec, head_spec, head_spec, head_spec, out_proj_spec, col_spec, col_spec, down_spec, P(None, None)), out_specs=(row_spec, cache_spec, cache_spec), check_vma=False)
```

```python
import functools
import jax
import jax.numpy as jnp
from jax import lax
from jax.experimental import pallas as pl
from jax.experimental.pallas import tpu as pltpu
from jax.sharding import PartitionSpec as P

ROPE_BASE = 500000.0
EPS = 1e-5
LOG2E = 1.4426950408889634
NEG = -1e30
MESH = pl.DeviceIdType.MESH
TOK, DM, QW, LN, HD = 256, 2048, 1024, 128, 64
F32 = jnp.float32
BF16 = jnp.bfloat16
VMEM_LIMIT = 62 * 1024 * 1024

DIM_ORDER = (((0, 1, 2), (0, 1, 2), (1, 2, 0), (2, 0, 1)), ((0, 1, 2), (1, 2, 0), (1, 2, 0), (2, 0, 1)))


def rope_tables(positions, head_dim):
    half_dim = head_dim // 2
    inv_freq = ROPE_BASE ** (-(jnp.arange(half_dim, dtype=F32) * 2.0 / head_dim))
    angles = positions.astype(F32)[None, :] * inv_freq[:, None]
    return jnp.cos(angles), jnp.sin(angles)


class Place:
    def __init__(self):
        self.seq = lax.axis_index('seq')
        self.head = lax.axis_index('head')
        self.xyz = (self.seq % 4, (self.seq // 4) % 4, self.seq // 16)
        self.mem = tuple(c // 2 for c in self.xyz)
        self.cls = tuple(((c + 1) // 2) % 2 for c in self.xyz)
        self.core = (self.mem[0] + self.mem[1]) % 2
        self.kv_local = 2 * self.mem[1] + self.mem[0]
        self.member = 2 * self.mem[2] + self.mem[0]

    def is_self(self):
        same_z = 1 - lax.rem(self.head + self.mem[2], 2)
        same_c = 1 - lax.rem(self.head + self.core, 2)
        return same_z * same_c

    def at(self, mem, cls):
        cs = [m * 3 + c * (1 - 2 * m) for m, c in zip(mem, cls)]
        return cs[2] * 16 + cs[1] * 4 + cs[0]

    def target(self, t):
        return self.at((t % 2, t // 2, self.head), self.cls)

    def source_mem(self, i):
        mx, mz = i % 2, i // 2
        return (mx, (mx + self.head) % 2, mz)

    def source(self, i, flips=()):
        cls = [1 - c if d in flips else c for d, c in enumerate(self.cls)]
        return self.at(self.source_mem(i), cls)

    def partner(self, dim):
        cls = [1 - c if d == dim else c for d, c in enumerate(self.cls)]
        return self.at(self.mem, cls)

    def dev(self, seq, head):
        return {'seq': seq, 'head': head}


N_TILES = 16
N_BEFORE = 14
NB = 4
TK = NB * TOK
HALF = NB * LN
RC = 16
NT = (((1,), (1,)), ((), ()))


def fold_max(x):
    return jnp.max(x.reshape(x.shape[0] // RC, RC, x.shape[1]), axis=0)


def fold_sum(x):
    return jnp.sum(x.reshape(x.shape[0] // RC, RC, x.shape[1]), axis=0)


def attn_logits(first, c, kv_all, qa, qb, sbuf, off, mx_ref, moff):
    cols = pl.ds(c * TOK, TOK)
    keys = kv_all[pl.ds(first, NB), 0:LN, :].reshape(HALF, LN)
    sa = jnp.dot(keys, qa[:, cols], preferred_element_type=F32) * (LOG2E / 8.0)
    sb = jnp.dot(keys, qb[:, cols], preferred_element_type=F32) * (LOG2E / 8.0)
    sbuf[pl.ds(off, HALF), cols] = sa
    sbuf[pl.ds(off + HALF, HALF), cols] = sb
    mx_ref[pl.ds(moff, RC), cols] = jnp.maximum(fold_max(sa), fold_max(sb))


def attn_update(cols, mx, parts, vTs, m_ref, l_ref, acc_ref):
    m_old = m_ref[0:1, cols]
    m_new = jnp.maximum(m_old, jnp.max(mx, axis=0, keepdims=True))
    alpha = jnp.exp2(m_old - m_new)
    m_ref[:, cols] = jnp.broadcast_to(m_new, (8, TOK))
    lsum = l_ref[:, cols] * alpha
    ps = []
    for s in parts:
        p = jnp.exp2(s - m_new)
        lsum = lsum + fold_sum(p)
        ps.append(p.astype(BF16))
    l_ref[:, cols] = lsum
    pv = jnp.dot(jnp.concatenate(vTs, axis=1), jnp.concatenate(ps, axis=0), preferred_element_type=F32)
    acc_ref[:, cols] = acc_ref[:, cols] * alpha + pv


def values_of(kv_all, first, blocks):
    return [kv_all[first + b, LN + HD * h:192 + HD * h, :] for h in range(2) for b in range(blocks)]


def attn_tail(first, t, kv_all, sbuf, off, m_ref, l_ref, acc_ref):
    def col(c, carry):
        cols = pl.ds(pl.multiple_of(c * TOK, TOK), TOK)
        ti = lax.broadcasted_iota(jnp.int32, (LN, TOK), 1)
        ki = lax.broadcasted_iota(jnp.int32, (LN, TOK), 0)
        parts = []
        for h in range(2):
            base = pl.multiple_of(off + h * HALF, LN)
            if t > 0:
                parts.append(sbuf[pl.ds(base, t * LN), cols])
            parts.append(jnp.where(ki + h * LN <= ti, sbuf[pl.ds(base + t * LN, LN), cols], NEG))
        mx = functools.reduce(jnp.maximum, [fold_max(p) for p in parts])
        attn_update(cols, mx, parts, values_of(kv_all, first, t + 1), m_ref, l_ref, acc_ref)
        return carry

    lax.fori_loop(0, 4, col, 0)


def attn_block(pos, qT, kv_all, store, qa, qb, m_ref, l_ref, acc_ref, sbuf, mx_ref):
    zero = jnp.zeros((HD, TOK), BF16)
    for g in range(4):
        q = qT[g * HD:(g + 1) * HD, :]
        cols = pl.ds(g * TOK, TOK)
        qa[:, cols] = jnp.concatenate([q, zero], axis=0)
        qb[:, cols] = jnp.concatenate([zero, q], axis=0)
    m_ref[:] = jnp.full_like(m_ref, NEG)
    l_ref[:] = jnp.zeros_like(l_ref)
    acc_ref[:] = jnp.zeros_like(acc_ref)
    groups = pos // NB
    for c in range(4):
        attn_logits(0, c, kv_all, qa, qb, sbuf, 0, mx_ref, 0)

    def one(n, p):
        for c in range(4):
            attn_logits((n + 1) * NB, c, kv_all, qa, qb, sbuf, (1 - p) * TK, mx_ref, (1 - p) * RC)
            cols = pl.ds(c * TOK, TOK)
            attn_update(cols, mx_ref[pl.ds(p * RC, RC), cols], [sbuf[pl.ds(p * TK, TK), cols]], values_of(kv_all, n * NB, NB), m_ref, l_ref, acc_ref)

    def pair(i, carry):
        one(2 * i, 0)
        one(2 * i + 1, 1)
        return carry

    lax.fori_loop(0, groups // 2, pair, 0)

    @pl.when(groups % 2 == 1)
    def _():
        one(groups - 1, 0)
    for t in range(NB):
        @pl.when(pos % NB == t)
        def _():
            attn_tail(groups * NB, t, kv_all, sbuf, (groups % 2) * TK, m_ref, l_ref, acc_ref)
    oT = acc_ref[:] / jnp.sum(l_ref[:], axis=0, keepdims=True)
    halves = []
    for g in range(0, 4, 2):
        two = jnp.concatenate([oT[:, g * TOK:(g + 1) * TOK], oT[:, (g + 1) * TOK:(g + 2) * TOK]], axis=0)
        halves.append(two.T.astype(BF16))
    store(jnp.concatenate(halves, axis=1))


def layer_kernel(layer, x_ref, gain_ref, cosT_ref, sinT_ref, wq, wk, wv, wg, wu, wd, wo, out_ref, kT_ref, vT_ref,
                 h_ref, q_send, kv_send, q_all, kv_all, o_send, o_full, mlp, part, part_in, wqb, wkb, wvb, wgb, wub, wdb, wob,
                 qa, qb, m_ref, l_ref, acc_ref, sbuf, mx_ref,
                 wsem, msem, osem, skv, sq, sag, sdd, so, sp, rkv, rq, rag, rdd, ro, rp):
    me = Place()
    sib = 1 - me.head
    flag = me.is_self()

    def s_self(i):
        return flag * (1 - lax.rem(i // 2 + me.mem[2], 2)) * (1 - lax.rem(i % 2 + me.mem[0], 2))

    def t_self(t):
        return flag * (1 - lax.rem(t // 2 + me.mem[1], 2)) * (1 - lax.rem(t % 2 + me.mem[0], 2))

    def remote(src, dst, ssem, rsem, seq, head):
        return pltpu.make_async_remote_copy(src_ref=src, dst_ref=dst, send_sem=ssem, recv_sem=rsem, device_id=me.dev(seq, head), device_id_type=MESH)

    barrier = pltpu.get_barrier_semaphore()
    for i in range(4):
        @pl.when(s_self(i) == 0)
        def _():
            pl.semaphore_signal(barrier, inc=1, device_id=me.dev(me.source(i), me.mem[2]), device_id_type=MESH)
    for t in range(4):
        @pl.when(t_self(t) == 0)
        def _():
            pl.semaphore_signal(barrier, inc=1, device_id=me.dev(me.target(t), me.core), device_id_type=MESH)
    for d in range(3):
        pl.semaphore_signal(barrier, inc=1, device_id=me.dev(me.partner(d), me.head), device_id_type=MESH)
    pl.semaphore_signal(barrier, inc=1, device_id=me.dev(me.seq, sib), device_id_type=MESH)

    cps = [pltpu.make_async_copy(wk.at[layer], wkb, wsem.at[0]), pltpu.make_async_copy(wv.at[layer], wvb, wsem.at[1])]
    for t in range(4):
        cps.append(pltpu.make_async_copy(wq.at[layer, pl.ds(t * TOK, TOK)], wqb.at[t], wsem.at[2 + t]))
    for c in cps:
        c.start()

    def tile_copies(n, slot):
        off = pl.multiple_of(n * TOK, TOK)
        return (pltpu.make_async_copy(wg.at[layer, :, pl.ds(off, TOK)], wgb.at[slot], msem.at[slot, 0]),
                pltpu.make_async_copy(wu.at[layer, :, pl.ds(off, TOK)], wub.at[slot], msem.at[slot, 1]),
                pltpu.make_async_copy(wd.at[layer, pl.ds(off, TOK)], wdb.at[slot], msem.at[slot, 2]))

    for n in range(3):
        for c in tile_copies(n, n):
            c.start()
    wo_cps = [pltpu.make_async_copy(wo.at[layer, pl.ds(t * TOK, TOK)], wob.at[t], osem.at[t]) for t in range(4)]

    xf = x_ref[:].astype(F32)
    inv = lax.rsqrt(jnp.mean(xf * xf, axis=-1, keepdims=True) + EPS)
    h_ref[:] = (xf * inv * gain_ref[layer:layer + 1, :].astype(F32)).astype(BF16)

    cosT, sinT = cosT_ref[:], sinT_ref[:]

    def rope(a):
        lo, hi = a[0:32], a[32:HD]
        return jnp.concatenate([lo * cosT - hi * sinT, hi * cosT + lo * sinT], axis=0)

    def project(w):
        return lax.dot_general(w, h_ref[:], NT, preferred_element_type=F32).astype(BF16)

    cps[0].wait()
    kT = project(wkb[:]).astype(F32)
    for t in range(4):
        k = rope(kT[t * HD:(t + 1) * HD]).astype(BF16)
        kT_ref[t * HD:(t + 1) * HD, :] = k
        kf = k.astype(F32)
        kv_send[t, 0:LN, :] = jnp.concatenate([kf[:, 0:LN], kf[:, LN:TOK]], axis=0).T.astype(BF16)
    cps[1].wait()
    vT = project(wvb[:])
    vT_ref[:] = vT
    for t in range(4):
        kv_send[t, LN:192, :] = vT[t * HD:(t + 1) * HD, 0:LN]
        kv_send[t, 192:TOK, :] = vT[t * HD:(t + 1) * HD, LN:TOK]

    pl.semaphore_wait(barrier, 12 - 2 * flag)

    def kv_copy(t):
        return remote(kv_send.at[t], kv_all.at[me.seq], skv.at[t], rkv.at[me.member], me.target(t), me.core)

    def q_copy(t):
        return remote(q_send.at[t], q_all.at[me.member], sq.at[t], rq.at[me.member], me.target(t), me.core)

    def send_all(make, src, dst, idx):
        for t in range(4):
            @pl.when(t_self(t) == 0)
            def _():
                make(t).start()

            @pl.when(t_self(t) == 1)
            def _():
                dst[idx] = src[t]

    send_all(kv_copy, kv_send, kv_all, me.seq)

    for t in range(4):
        cps[2 + t].wait()
        qT = project(wqb[t]).astype(F32)
        for g in range(4):
            q_send[t, g * HD:(g + 1) * HD, :] = rope(qT[g * HD:(g + 1) * HD]).astype(BF16)
    send_all(q_copy, q_send, q_all, me.member)

    def plan(core, i, k):
        d1, d2, d3 = DIM_ORDER[core][i]
        return ((d1, ()), (d2, ()), (d2, (d1,)), (d3, ()), (d3, (d1,)), (d3, (d2,)), (d3, (d1, d2)))[k]

    def got(core, i, k):
        dim, flips = plan(core, i, k)
        return tuple(flips) + (dim,)

    def ag(core, i, k):
        dim, flips = plan(core, i, k)
        block = kv_all.at[me.source(i, flips)]
        return remote(block, block, sag.at[i, k], rag.at[i, k], me.partner(dim), me.head)

    def ag_recv(core, i, k):
        block = kv_all.at[me.source(i, got(core, i, k))]
        remote(block, block, sag.at[i, k], rag.at[i, k], me.seq, sib).wait_recv()

    def dd(pos, i, k):
        return remote(kv_all.at[pos], kv_all.at[pos], sdd.at[i, k], rdd.at[i, k], me.seq, sib)

    def relay(core, i, k):
        dd(me.source(i, got(core, i, k)), i, k + 1).start()

    def per_core(fn, *a):
        for core in range(2):
            @pl.when(me.head == core)
            def _():
                fn(core, *a)

    def step1(core, group):
        for i in group:
            @pl.when(s_self(i) == 0)
            def _():
                remote(kv_send.at[0], kv_all.at[me.source(i)], skv.at[0], rkv.at[i], me.seq, sib).wait_recv()
            ag(core, i, 0).start()
        for k in (1, 3):
            for i in group:
                ag(core, i, k).start()
        for i in group:
            dd(me.source(i), i, 0).start()

    def step2(core, group):
        for i in group:
            ag_recv(core, i, 0)
            ag(core, i, 2).start()
            ag(core, i, 4).start()
            relay(core, i, 0)
        for i in group:
            ag_recv(core, i, 1)
            ag(core, i, 5).start()
            relay(core, i, 1)

    def step3(core, group):
        for i in group:
            ag_recv(core, i, 2)
            ag(core, i, 6).start()
            relay(core, i, 2)

    def step4(core, group):
        for k in range(3, 7):
            for i in group:
                ag_recv(core, i, k)
                relay(core, i, k)

    def sibling_blocks(core, group):
        other = 1 - core
        for k in range(8):
            for i in group:
                mx, mz = i % 2, i // 2
                flips = () if k == 0 else got(other, i, k - 1)
                cls = [1 - c if d in flips else c for d, c in enumerate(me.cls)]
                dd(me.at((mx, (mx + other) % 2, mz), cls), i, k).wait_recv()

    mlp[:] = jnp.zeros_like(mlp)
    low, high = (0, 1), (2, 3)
    events = EVENTS

    def tile(n, carry):
        slot = n % 3
        for c in tile_copies(n, slot):
            c.wait()
        for at, name, group in events:
            @pl.when(n == at)
            def _():
                per_core({1: step1, 2: step2, 3: step3, 4: step4}[name], group)
        g = jnp.dot(h_ref[:], wgb[slot], preferred_element_type=F32)
        u = jnp.dot(h_ref[:], wub[slot], preferred_element_type=F32)
        hid = (g * jax.nn.sigmoid(g) * u).astype(BF16)
        mlp[:] += jnp.dot(hid, wdb[slot], preferred_element_type=F32)

        @pl.when(n + 3 < N_TILES)
        def _():
            for c in tile_copies(n + 3, slot):
                c.start()
        return carry

    lax.fori_loop(0, N_BEFORE, tile, 0)
    for c in wo_cps:
        c.start()
    per_core(step4, low)
    per_core(sibling_blocks, low)
    for i in range(4):
        @pl.when(s_self(i) == 0)
        def _():
            remote(q_send.at[0], q_all.at[i], sq.at[0], rq.at[i], me.seq, sib).wait_recv()

    def o_copy(i):
        return remote(o_send.at[i], o_full.at[me.kv_local], so.at[i], ro.at[me.kv_local], me.source(i), me.mem[2])

    def query(n, carry):
        first = (1 - n % 2) * me.head + (n % 2) * (1 - me.head)
        i = 2 * (n // 2) + first

        @pl.when(n == 2)
        def _():
            per_core(sibling_blocks, high)

        def store(val):
            o_send[i] = val
        attn_block(me.source(i), q_all[i], kv_all, store, qa, qb, m_ref, l_ref, acc_ref, sbuf, mx_ref)

        @pl.when(n == 0)
        def _():
            per_core(step4, high)
        own = s_self(i)

        @pl.when(own == 0)
        def _():
            o_copy(i).start()

        @pl.when(own == 1)
        def _():
            o_full[me.kv_local] = o_send[i]
        return carry

    lax.fori_loop(0, 4, query, 0)
    lax.fori_loop(N_BEFORE, N_TILES, tile, 0)

    for c in wo_cps:
        c.wait()
    for t in range(4):
        @pl.when(t_self(t) == 0)
        def _():
            remote(o_send.at[0], o_full.at[t], so.at[0], ro.at[t], me.seq, sib).wait_recv()

    def p_copy(n):
        return remote(part.at[n], part_in.at[n], sp.at[n], rp.at[n], me.seq, sib)

    for n in range(8):
        cols = pl.ds(n * TOK, TOK)
        heads = jnp.concatenate([o_full[t] for t in range(4)], axis=1)
        w = jnp.concatenate([wob[t, :, cols] for t in range(4)], axis=0)
        part[n] = mlp[:, cols] + jnp.dot(heads, w, preferred_element_type=F32)
        p_copy(n).start()
    for n in range(8):
        cols = pl.ds(n * TOK, TOK)
        p_copy(n).wait_recv()
        y = (part[n] + part_in[n]).astype(BF16)
        out_ref[:, cols] = (x_ref[:, cols].astype(F32) + y.astype(F32)).astype(BF16)

    for t in range(4):
        @pl.when(t_self(t) == 0)
        def _():
            kv_copy(t).wait_send()
            q_copy(t).wait_send()

    def sent(core):
        for i in range(4):
            for k in range(7):
                ag(core, i, k).wait_send()
            for k in range(8):
                dd(me.source(i), i, k).wait_send()
    per_core(sent)
    for i in range(4):
        @pl.when(s_self(i) == 0)
        def _():
            o_copy(i).wait_send()
    for n in range(8):
        p_copy(n).wait_send()


EVENTS = ((3, 1, (0, 1)), (6, 2, (0, 1)), (6, 1, (2, 3)), (9, 3, (0, 1)), (9, 2, (2, 3)), (12, 3, (2, 3)))


SCRATCH = [
    pltpu.VMEM((TOK, DM), BF16), pltpu.VMEM((4, TOK, TOK), BF16), pltpu.VMEM((4, TOK, LN), BF16),
    pltpu.VMEM((4, TOK, TOK), BF16), pltpu.VMEM((HD, TOK, LN), BF16), pltpu.VMEM((4, TOK, TOK), BF16), pltpu.VMEM((4, TOK, TOK), BF16),
    pltpu.VMEM((TOK, DM), F32), pltpu.VMEM((8, TOK, TOK), F32), pltpu.VMEM((8, TOK, TOK), F32),
    pltpu.VMEM((4, TOK, DM), BF16), pltpu.VMEM((TOK, DM), BF16), pltpu.VMEM((TOK, DM), BF16),
    pltpu.VMEM((3, DM, TOK), BF16), pltpu.VMEM((3, DM, TOK), BF16), pltpu.VMEM((3, TOK, DM), BF16), pltpu.VMEM((4, TOK, DM), BF16),
    pltpu.VMEM((LN, QW), BF16), pltpu.VMEM((LN, QW), BF16), pltpu.VMEM((8, QW), F32), pltpu.VMEM((RC, QW), F32), pltpu.VMEM((HD, QW), F32),
    pltpu.VMEM((2 * TK, QW), F32), pltpu.VMEM((2 * RC, QW), F32),
] + [pltpu.SemaphoreType.DMA(s) for s in ((6,), (3, 3), (4,), (4,), (4,), (4, 7), (4, 8), (4,), (8,), (4,), (4,), (4, 7), (4, 8), (4,), (8,))]


def vm():
    return pl.BlockSpec(memory_space=pltpu.VMEM)


def hbm():
    return pl.BlockSpec(memory_space=pl.ANY)


def sds(shape, dtype):
    return jax.ShapeDtypeStruct(shape, dtype)


def dma(*shape):
    return pltpu.SemaphoreType.DMA(shape)


def solution(mesh):
    row_spec = P(('batch', 'seq'), None)
    pos_spec = P(('batch', 'seq'))
    head_spec = P(None, None, 'head', None)
    out_proj_spec = P(None, 'head', None, None)
    col_spec = P(None, None, 'head')
    down_spec = P(None, 'head', None)
    cache_spec = P(None, ('batch', 'seq'), 'head', None)

    def local_forward(x, pos, w_q, w_k, w_v, w_o, w_gate, w_up, w_down, gain):
        cosT, sinT = rope_tables(pos, HD)
        wq = w_q.transpose(0, 2, 3, 1).reshape(2, QW, DM)
        wk = w_k.transpose(0, 2, 3, 1).reshape(2, TOK, DM)
        wv = w_v.transpose(0, 2, 3, 1).reshape(2, TOK, DM)
        wo = w_o.reshape(2, QW, DM)
        ks, vs = [], []
        for layer in range(2):
            x, kT, vT = pl.pallas_call(
                functools.partial(layer_kernel, layer),
                out_shape=(sds((TOK, DM), BF16), sds((TOK, TOK), BF16), sds((TOK, TOK), BF16)),
                in_specs=[vm()] * 4 + [hbm()] * 7,
                out_specs=[vm()] * 3,
                scratch_shapes=SCRATCH,
                compiler_params=pltpu.CompilerParams(collective_id=layer, has_side_effects=True, vmem_limit_bytes=VMEM_LIMIT),
                name=f'layer{layer}',
            )(x, gain, cosT, sinT, wq, wk, wv, w_gate, w_up, w_down, wo)
            ks.append(kT)
            vs.append(vT)
        k_cache = jnp.stack(ks).reshape(2, 4, HD, TOK).transpose(0, 3, 1, 2)
        v_cache = jnp.stack(vs).reshape(2, 4, HD, TOK).transpose(0, 3, 1, 2)
        return x, k_cache, v_cache

    return jax.shard_map(local_forward, mesh=mesh, in_specs=(row_spec, pos_spec, head_spec, head_spec, head_spec, out_proj_spec, col_spec, col_spec, down_spec, P(None, None)), out_specs=(row_spec, cache_spec, cache_spec), check_vma=False)
```

```python
import functools
import jax
import jax.numpy as jnp
from jax import lax
from jax.experimental import pallas as pl
from jax.experimental.pallas import tpu as pltpu
from jax.sharding import PartitionSpec as P

ROPE_BASE = 500000.0
EPS = 1e-5
LOG2E = 1.4426950408889634
NEG = -1e30
MESH = pl.DeviceIdType.MESH
TOK, DM, QW, LN, HD = 256, 2048, 1024, 128, 64
F32 = jnp.float32
BF16 = jnp.bfloat16
VMEM_LIMIT = 62 * 1024 * 1024

STRIDE = (1, 4, 16)
N_TILES = 16
LAST_BEFORE = 14
NB = 4
TK = NB * TOK
HALF = NB * LN
RC = 16
NT = (((1,), (1,)), ((), ()))
LOW, HIGH = (0, 1), (2, 3)
SENDS = ((0, ()), (1, ()), (1, (0,)), (2, ()), (2, (0,)), (2, (1,)), (2, (0, 1)))


def rope_tables(positions, head_dim):
    half_dim = head_dim // 2
    inv_freq = ROPE_BASE ** (-(jnp.arange(half_dim, dtype=F32) * 2.0 / head_dim))
    angles = positions.astype(F32)[None, :] * inv_freq[:, None]
    return jnp.cos(angles), jnp.sin(angles)


class Place:
    def __init__(self):
        self.seq = lax.axis_index('seq')
        self.head = lax.axis_index('head')
        self.xyz = (self.seq % 4, (self.seq // 4) % 4, self.seq // 16)
        self.mem = tuple(c // 2 for c in self.xyz)
        self.cls = tuple(((c + 1) // 2) % 2 for c in self.xyz)
        self.core = (self.mem[0] + self.mem[1]) % 2
        self.kv_local = 2 * self.mem[1] + self.mem[0]
        self.member = 2 * self.mem[2] + self.mem[0]
        same_z = 1 - lax.rem(self.head + self.mem[2], 2)
        self.flag = same_z * (1 - lax.rem(self.head + self.core, 2))

    def at(self, mem):
        cs = [m * 3 + c * (1 - 2 * m) for m, c in zip(mem, self.cls)]
        return cs[2] * 16 + cs[1] * 4 + cs[0]

    def target(self, t):
        return self.at((t % 2, t // 2, self.head))

    def source_mem(self, i):
        mx = i % 2
        return (mx, (mx + self.head) % 2, i // 2)

    def source(self, i):
        return self.at(self.source_mem(i))

    def steps(self, i, mem):
        d = [(1 - 2 * c) * (1 - 2 * m) * s for c, m, s in zip(self.cls, mem, STRIDE)]
        turns = [d[k:] + d[:k] for k in range(3)]
        if i == 1:
            return [a * (1 - self.head) + b * self.head for a, b in zip(turns[0], turns[1])]
        return turns[max(i - 1, 0)]

    def s_self(self, i):
        return self.flag * (1 - lax.rem(i // 2 + self.mem[2], 2)) * (1 - lax.rem(i % 2 + self.mem[0], 2))

    def t_self(self, t):
        return self.flag * (1 - lax.rem(t // 2 + self.mem[1], 2)) * (1 - lax.rem(t % 2 + self.mem[0], 2))


def fold_max(x):
    return jnp.max(x.reshape(x.shape[0] // RC, RC, x.shape[1]), axis=0)


def fold_sum(x):
    return jnp.sum(x.reshape(x.shape[0] // RC, RC, x.shape[1]), axis=0)


def attn_logits(first, c, kv_all, qa, qb, sbuf, off, mx_ref, moff):
    cols = pl.ds(c * TOK, TOK)
    keys = kv_all[pl.ds(first, NB), 0:LN, :].reshape(HALF, LN)
    sa = jnp.dot(keys, qa[:, cols], preferred_element_type=F32) * (LOG2E / 8.0)
    sb = jnp.dot(keys, qb[:, cols], preferred_element_type=F32) * (LOG2E / 8.0)
    sbuf[pl.ds(off, HALF), cols] = sa
    sbuf[pl.ds(off + HALF, HALF), cols] = sb
    mx_ref[pl.ds(moff, RC), cols] = jnp.maximum(fold_max(sa), fold_max(sb))


def attn_update(cols, mx, parts, vTs, m_ref, l_ref, acc_ref):
    m_old = m_ref[0:1, cols]
    m_new = jnp.maximum(m_old, jnp.max(mx, axis=0, keepdims=True))
    alpha = jnp.exp2(m_old - m_new)
    m_ref[:, cols] = jnp.broadcast_to(m_new, (8, TOK))
    lsum = l_ref[:, cols] * alpha
    ps = []
    for s in parts:
        p = jnp.exp2(s - m_new)
        lsum = lsum + fold_sum(p)
        ps.append(p.astype(BF16))
    l_ref[:, cols] = lsum
    pv = jnp.dot(jnp.concatenate(vTs, axis=1), jnp.concatenate(ps, axis=0), preferred_element_type=F32)
    acc_ref[:, cols] = acc_ref[:, cols] * alpha + pv


def values_of(kv_all, first, blocks):
    return [kv_all[first + b, LN + HD * h:192 + HD * h, :] for h in range(2) for b in range(blocks)]


def attn_tail(first, t, kv_all, sbuf, off, m_ref, l_ref, acc_ref):
    def col(c, carry):
        cols = pl.ds(pl.multiple_of(c * TOK, TOK), TOK)
        ti = lax.broadcasted_iota(jnp.int32, (LN, TOK), 1)
        ki = lax.broadcasted_iota(jnp.int32, (LN, TOK), 0)
        parts = []
        for h in range(2):
            base = pl.multiple_of(off + h * HALF, LN)
            if t > 0:
                parts.append(sbuf[pl.ds(base, t * LN), cols])
            parts.append(jnp.where(ki + h * LN <= ti, sbuf[pl.ds(base + t * LN, LN), cols], NEG))
        mx = functools.reduce(jnp.maximum, [fold_max(p) for p in parts])
        attn_update(cols, mx, parts, values_of(kv_all, first, t + 1), m_ref, l_ref, acc_ref)
        return carry

    lax.fori_loop(0, 4, col, 0)


def attn_block(pos, qT, kv_all, store, qa, qb, m_ref, l_ref, acc_ref, sbuf, mx_ref):
    zero = jnp.zeros((HD, TOK), BF16)
    for g in range(4):
        q = qT[g * HD:(g + 1) * HD, :]
        cols = pl.ds(g * TOK, TOK)
        qa[:, cols] = jnp.concatenate([q, zero], axis=0)
        qb[:, cols] = jnp.concatenate([zero, q], axis=0)
    m_ref[:] = jnp.full_like(m_ref, NEG)
    l_ref[:] = jnp.zeros_like(l_ref)
    acc_ref[:] = jnp.zeros_like(acc_ref)
    groups = pos // NB
    for c in range(4):
        attn_logits(0, c, kv_all, qa, qb, sbuf, 0, mx_ref, 0)

    def one(n, p):
        for c in range(4):
            attn_logits((n + 1) * NB, c, kv_all, qa, qb, sbuf, (1 - p) * TK, mx_ref, (1 - p) * RC)
            cols = pl.ds(c * TOK, TOK)
            attn_update(cols, mx_ref[pl.ds(p * RC, RC), cols], [sbuf[pl.ds(p * TK, TK), cols]], values_of(kv_all, n * NB, NB), m_ref, l_ref, acc_ref)

    def pair(i, carry):
        one(2 * i, 0)
        one(2 * i + 1, 1)
        return carry

    lax.fori_loop(0, groups // 2, pair, 0)

    @pl.when(groups % 2 == 1)
    def _():
        one(groups - 1, 0)
    for t in range(NB):
        @pl.when(pos % NB == t)
        def _():
            attn_tail(groups * NB, t, kv_all, sbuf, (groups % 2) * TK, m_ref, l_ref, acc_ref)
    oT = acc_ref[:] / jnp.sum(l_ref[:], axis=0, keepdims=True)
    halves = []
    for g in range(0, 4, 2):
        two = jnp.concatenate([oT[:, g * TOK:(g + 1) * TOK], oT[:, (g + 1) * TOK:(g + 2) * TOK]], axis=0)
        halves.append(two.T.astype(BF16))
    store(jnp.concatenate(halves, axis=1))


def stack_kernel(x_hbm, gain_ref, cos_hbm, sin_hbm, wq, wk, wv, wg, wu, wd, wo, x_ref, k_ref, v_ref,
                 cosT, sinT, h_ref, q_send, kv_send, q_all, kv_all, o_send, o_full, mlp, part_in, hid, wqb, wkvb, wgb, wub, wdb, wob,
                 qa, qb, m_ref, l_ref, acc_ref, sbuf, mx_ref,
                 xsem, wsem, msem, osem, skv, sq, sag, sdd, so, sp, rkv, rq, rag, rdd, ro, rp):
    me = Place()
    sib = 1 - me.head

    def remote(src, dst, ssem, rsem, seq, head):
        return pltpu.make_async_remote_copy(src_ref=src, dst_ref=dst, send_sem=ssem, recv_sem=rsem, device_id={'seq': seq, 'head': head}, device_id_type=MESH)

    def for_others(is_self, fn):
        for i in range(4):
            @pl.when(is_self(i) == 0)
            def _():
                fn(i)

    barrier = pltpu.get_barrier_semaphore()

    def hello(seq, head):
        pl.semaphore_signal(barrier, inc=1, device_id={'seq': seq, 'head': head}, device_id_type=MESH)

    for_others(me.s_self, lambda i: hello(me.source(i), me.mem[2]))
    for_others(me.t_self, lambda t: hello(me.target(t), me.core))
    for step in me.steps(0, me.mem):
        hello(me.seq + step, me.head)
    hello(me.seq, sib)

    start_cps = [pltpu.make_async_copy(x_hbm, x_ref, xsem.at[0]), pltpu.make_async_copy(cos_hbm, cosT, xsem.at[1]), pltpu.make_async_copy(sin_hbm, sinT, xsem.at[2])]

    def proj_copies(layer):
        return (pltpu.make_async_copy(wk.at[layer], wkvb.at[pl.ds(0, TOK)], wsem.at[0]), pltpu.make_async_copy(wv.at[layer], wkvb.at[pl.ds(TOK, TOK)], wsem.at[1]), pltpu.make_async_copy(wq.at[layer], wqb, wsem.at[2]))

    def gu_copies(layer, n):
        off = pl.multiple_of(n * TOK, TOK)
        slot = n % 3
        return (pltpu.make_async_copy(wg.at[layer, :, pl.ds(off, TOK)], wgb.at[slot], msem.at[0, slot]), pltpu.make_async_copy(wu.at[layer, :, pl.ds(off, TOK)], wub.at[slot], msem.at[1, slot]))

    def d_copy(layer, n):
        return pltpu.make_async_copy(wd.at[layer, pl.ds(pl.multiple_of(n * TOK, TOK), TOK)], wdb.at[n % 3], msem.at[2, n % 3])

    def first_tiles(layer):
        for n in range(3):
            for c in gu_copies(layer, n):
                c.start()
        for n in range(2):
            d_copy(layer, n).start()

    for c in start_cps:
        c.start()
    for c in proj_copies(0):
        c.start()
    first_tiles(0)
    for c in start_cps:
        c.wait()

    def rope(a):
        lo, hi = a[0:32], a[32:HD]
        return jnp.concatenate([lo * cosT[:] - hi * sinT[:], hi * cosT[:] + lo * sinT[:]], axis=0)

    def project(w):
        return lax.dot_general(w, h_ref[:], NT, preferred_element_type=F32).astype(BF16)

    def layer_body(layer, carry):
        kv = kv_all.at[layer]
        xf = x_ref[:].astype(F32)
        inv = lax.rsqrt(jnp.mean(xf * xf, axis=-1, keepdims=True) + EPS)
        gain = jnp.where(layer == 0, gain_ref[0:1, :].astype(F32), gain_ref[1:2, :].astype(F32))
        h_ref[:] = (xf * inv * gain).astype(BF16)

        w_cps = proj_copies(layer)
        w_cps[0].wait()
        w_cps[1].wait()
        kvT = project(wkvb[:])
        for t in range(4):
            k = rope(kvT[t * HD:(t + 1) * HD].astype(F32)).astype(BF16)
            k_ref[layer, t * HD:(t + 1) * HD, :] = k
            kf = k.astype(F32)
            kv_send[layer, t, 0:LN, :] = jnp.concatenate([kf[:, 0:LN], kf[:, LN:TOK]], axis=0).T.astype(BF16)
            v = kvT[TOK + t * HD:TOK + (t + 1) * HD]
            v_ref[layer, t * HD:(t + 1) * HD, :] = v
            kv_send[layer, t, LN:LN + HD, :] = v[:, 0:LN]
            kv_send[layer, t, LN + HD:TOK, :] = v[:, LN:TOK]

        @pl.when(layer == 0)
        def _():
            pl.semaphore_wait(barrier, 12 - 2 * me.flag)

        def kv_copy(t):
            return remote(kv_send.at[layer, t], kv.at[me.seq], skv.at[layer, t], rkv.at[layer, me.member], me.target(t), me.core)

        def q_copy(t):
            return remote(q_send.at[layer, t], q_all.at[layer, me.member], sq.at[layer, t], rq.at[layer, me.member], me.target(t), me.core)

        for_others(me.t_self, lambda t: kv_copy(t).start())
        for t in range(4):
            @pl.when(me.t_self(t) == 1)
            def _():
                kv[me.seq] = kv_send[layer, t]

        w_cps[2].wait()
        qT = project(wqb[:])
        for g in range(16):
            q_send[layer, g // 4, (g % 4) * HD:(g % 4 + 1) * HD, :] = rope(qT[g * HD:(g + 1) * HD].astype(F32)).astype(BF16)
        for_others(me.t_self, lambda t: q_copy(t).start())
        for t in range(4):
            @pl.when(me.t_self(t) == 1)
            def _():
                q_all[layer, me.member] = q_send[layer, t]

        def place_of(i, crossed):
            steps = me.steps(i, me.source_mem(i))
            return functools.reduce(lambda a, d: a + steps[d], crossed, me.source(i))

        def ag(i, k):
            dim, crossed = SENDS[k]
            block = kv.at[place_of(i, crossed)]
            return remote(block, block, sag.at[layer], rag.at[layer, i, k], me.seq + me.steps(i, me.mem)[dim], me.head)

        def relay(i, crossed):
            block = kv.at[place_of(i, crossed)]
            remote(block, block, sdd.at[layer], rdd.at[layer, i // 2], me.seq, sib).start()

        def arrived(i, k):
            dim, crossed = SENDS[k]
            block = kv.at[place_of(i, crossed + (dim,))]
            remote(block, block, sag.at[layer], rag.at[layer, i, k], me.seq, sib).wait_recv()
            relay(i, crossed + (dim,))

        def step_own(group):
            for i in group:
                @pl.when(me.s_self(i) == 0)
                def _():
                    remote(kv_send.at[layer, 0], kv.at[me.source(i)], skv.at[layer, 0], rkv.at[layer, i], me.seq, sib).wait_recv()
            for k in (0, 1, 3):
                for i in group:
                    ag(i, k).start()
            for i in group:
                relay(i, ())

        def step_on(group, k, nexts):
            for i in group:
                arrived(i, k)
                for nxt in nexts:
                    ag(i, nxt).start()

        def step_end(group):
            for k in range(3, 7):
                step_on(group, k, ())

        def from_sibling(group):
            half = kv.at[pl.ds(0, 16)]
            remote(half, half, sdd.at[layer], rdd.at[layer, group[0] // 2], me.seq, sib).wait_recv()

        events = (
            (4, step_own, (LOW,)), (7, step_on, (LOW, 0, (2, 4))), (8, step_on, (LOW, 1, (5,))), (10, step_on, (LOW, 2, (6,))),
            (10, step_own, (HIGH,)), (13, step_end, (LOW,)), (14, step_on, (HIGH, 0, (2, 4))))

        def gate_up(n):
            g = jnp.dot(h_ref[:], wgb[n % 3], preferred_element_type=F32)
            u = jnp.dot(h_ref[:], wub[n % 3], preferred_element_type=F32)
            return (g * jax.nn.sigmoid(g) * u).astype(BF16)

        def add_down(hidden, n):
            d = jnp.dot(hidden, wdb[n % 3], preferred_element_type=F32)
            for c in range(8):
                mlp[layer, c] += d[:, c * TOK:(c + 1) * TOK]

        for c in range(8):
            mlp[layer, c] = jnp.zeros((TOK, TOK), F32)
        for c in gu_copies(layer, 0):
            c.wait()
        hid[:] = gate_up(0)
        for c in gu_copies(layer, 3):
            c.start()
        d_copy(layer, 2).start()

        def tile(n, carry):
            for c in gu_copies(layer, n):
                c.wait()
            d_copy(layer, n - 1).wait()
            for at, fn, fn_args in events:
                @pl.when(n == at)
                def _():
                    fn(*fn_args)
            before = hid[:]
            now = gate_up(n)
            add_down(before, n - 1)
            hid[:] = now

            @pl.when(n + 3 < N_TILES)
            def _():
                for c in gu_copies(layer, n + 3):
                    c.start()

            @pl.when(n + 2 < N_TILES)
            def _():
                d_copy(layer, n + 2).start()
            return carry

        lax.fori_loop(1, LAST_BEFORE + 1, tile, 0)
        o_cp = pltpu.make_async_copy(wo.at[layer], wob, osem.at[0])
        o_cp.start()

        @pl.when(layer == 0)
        def _():
            for c in proj_copies(1):
                c.start()
        step_on(HIGH, 1, (5,))
        step_on(HIGH, 2, (6,))
        from_sibling(LOW)
        for_others(me.s_self, lambda i: remote(q_send.at[layer, 0], q_all.at[layer, i], sq.at[layer, 0], rq.at[layer, i], me.seq, sib).wait_recv())

        def o_copy(i):
            return remote(o_send.at[layer, i], o_full.at[layer, me.kv_local], so.at[layer, i], ro.at[layer, me.kv_local], me.source(i), me.mem[2])

        def query(n, carry):
            i = 2 * (n // 2) + (1 - n % 2) * me.head + (n % 2) * (1 - me.head)

            @pl.when(n == 2)
            def _():
                from_sibling(HIGH)

            def store(val):
                o_send[layer, i] = val
            attn_block(me.source(i), q_all[layer, i], kv, store, qa, qb, m_ref, l_ref, acc_ref, sbuf, mx_ref)

            @pl.when(n == 0)
            def _():
                step_end(HIGH)

            @pl.when(me.s_self(i) == 0)
            def _():
                o_copy(i).start()

            @pl.when(me.s_self(i) == 1)
            def _():
                o_full[layer, me.kv_local] = o_send[layer, i]
            return carry

        lax.fori_loop(0, 4, query, 0)
        lax.fori_loop(LAST_BEFORE + 1, N_TILES, tile, 0)
        d_copy(layer, N_TILES - 1).wait()
        add_down(hid[:], N_TILES - 1)

        @pl.when(layer == 0)
        def _():
            first_tiles(1)

        o_cp.wait()
        for_others(me.t_self, lambda t: remote(o_send.at[layer, 0], o_full.at[layer, t], so.at[layer, 0], ro.at[layer, t], me.seq, sib).wait_recv())

        def p_copy(n):
            return remote(mlp.at[layer, n], part_in.at[layer, n], sp.at[layer], rp.at[layer, n], me.seq, sib)

        heads = jnp.concatenate([o_full[layer, t] for t in range(4)], axis=1)
        for n in range(0, 8, 2):
            d = jnp.dot(heads, wob[:, n * TOK:(n + 2) * TOK], preferred_element_type=F32)
            for e in range(2):
                mlp[layer, n + e] += d[:, e * TOK:(e + 1) * TOK]
                p_copy(n + e).start()
        for n in range(8):
            cols = pl.ds(n * TOK, TOK)
            p_copy(n).wait_recv()
            y = (mlp[layer, n] + part_in[layer, n]).astype(BF16)
            x_ref[:, cols] = (x_ref[:, cols].astype(F32) + y.astype(F32)).astype(BF16)
        return carry

    lax.fori_loop(0, 2, layer_body, 0)

    def drain(layer, carry):
        def gone(src, sem):
            remote(src, src, sem, rp.at[layer, 0], me.seq, sib).wait_send()

        for_others(me.t_self, lambda t: gone(kv_send.at[layer, t], skv.at[layer, t]))
        for_others(me.t_self, lambda t: gone(q_send.at[layer, t], sq.at[layer, t]))
        for_others(me.s_self, lambda i: gone(o_send.at[layer, i], so.at[layer, i]))
        gone(kv_all.at[layer, pl.ds(0, 28)], sag.at[layer])
        gone(kv_all.at[layer, pl.ds(0, 32)], sdd.at[layer])
        gone(mlp.at[layer], sp.at[layer])
        return carry

    lax.fori_loop(0, 2, drain, 0)


def vmem(*shape, dtype=BF16):
    return pltpu.VMEM(shape, dtype)


SCRATCH = [
    vmem(32, TOK, dtype=F32), vmem(32, TOK, dtype=F32), vmem(TOK, DM), vmem(2, 4, TOK, TOK), vmem(2, 4, TOK, LN), vmem(2, 4, TOK, TOK), vmem(2, HD, TOK, LN),
    vmem(2, 4, TOK, TOK), vmem(2, 4, TOK, TOK), vmem(2, 8, TOK, TOK, dtype=F32), vmem(2, 8, TOK, TOK, dtype=F32), vmem(TOK, TOK),
    vmem(QW, DM), vmem(2 * TOK, DM), vmem(3, DM, TOK), vmem(3, DM, TOK), vmem(3, TOK, DM), vmem(QW, DM),
    vmem(LN, QW), vmem(LN, QW), vmem(8, QW, dtype=F32), vmem(RC, QW, dtype=F32), vmem(HD, QW, dtype=F32), vmem(2 * TK, QW, dtype=F32), vmem(2 * RC, QW, dtype=F32),
] + [pltpu.SemaphoreType.DMA(s) for s in ((3,), (3,), (3, 3), (1,), (2, 4), (2, 4), (2,), (2,), (2, 4), (2,), (2, 4), (2, 4), (2, 4, 7), (2, 2), (2, 4), (2, 8))]


def solution(mesh):
    row_spec = P(('batch', 'seq'), None)
    pos_spec = P(('batch', 'seq'))
    head_spec = P(None, None, 'head', None)
    out_proj_spec = P(None, 'head', None, None)
    col_spec = P(None, None, 'head')
    down_spec = P(None, 'head', None)
    cache_spec = P(None, ('batch', 'seq'), 'head', None)
    in_vmem = pl.BlockSpec(memory_space=pltpu.VMEM)
    anywhere = pl.BlockSpec(memory_space=pl.ANY)

    def local_forward(x, pos, w_q, w_k, w_v, w_o, w_gate, w_up, w_down, gain):
        cosT, sinT = rope_tables(pos, HD)
        wq = w_q.transpose(0, 2, 3, 1).reshape(2, QW, DM)
        wk = w_k.transpose(0, 2, 3, 1).reshape(2, TOK, DM)
        wv = w_v.transpose(0, 2, 3, 1).reshape(2, TOK, DM)
        wo = w_o.reshape(2, QW, DM)
        x, kT, vT = pl.pallas_call(
            stack_kernel,
            out_shape=OUT_SHAPES,
            in_specs=[anywhere, in_vmem] + [anywhere] * 9,
            out_specs=(in_vmem,) * 3,
            scratch_shapes=SCRATCH,
            compiler_params=pltpu.CompilerParams(collective_id=0, has_side_effects=True, vmem_limit_bytes=VMEM_LIMIT),
            name='stack',
        )(x, gain, cosT, sinT, wq, wk, wv, w_gate, w_up, w_down, wo)
        k_cache = kT.reshape(2, 4, HD, TOK).transpose(0, 3, 1, 2)
        v_cache = vT.reshape(2, 4, HD, TOK).transpose(0, 3, 1, 2)
        return x, k_cache, v_cache

    return jax.shard_map(local_forward, mesh=mesh, in_specs=(row_spec, pos_spec, head_spec, head_spec, head_spec, out_proj_spec, col_spec, col_spec, down_spec, P(None, None)), out_specs=(row_spec, cache_spec, cache_spec), check_vma=False)


OUT_SHAPES = tuple(jax.ShapeDtypeStruct(s, BF16) for s in ((TOK, DM), (2, TOK, TOK), (2, TOK, TOK)))
```

```python
import functools
import jax
import jax.numpy as jnp
from jax import lax
from jax.experimental import pallas as pl
from jax.experimental.pallas import tpu as pltpu
from jax.sharding import PartitionSpec as P

ROPE_BASE = 500000.0
EPS = 1e-5
LOG2E = 1.4426950408889634
NEG = -1e30
MESH = pl.DeviceIdType.MESH
TOK, DM, QW, LN, HD = 256, 2048, 1024, 128, 64
F32 = jnp.float32
BF16 = jnp.bfloat16
VMEM_LIMIT = 62 * 1024 * 1024

STRIDE = (1, 4, 16)
N_TILES = 16
NB = 4
TK = NB * TOK
HALF = NB * LN
RC = 8
NT = (((1,), (1,)), ((), ()))
PARTS = ((0,), (1,), (2, 3))
SENDS = ((0, ()), (1, ()), (1, (0,)), (2, ()), (2, (0,)), (2, (1,)), (2, (0, 1)))
SECOND, THIRD = (1, 2), (3, 4, 5, 6)
NEXT = ((2, 4), (5,), (6,), (), (), (), ())
FOUR = range(4)


def rope_tables(positions, head_dim):
    half_dim = head_dim // 2
    inv_freq = ROPE_BASE ** (-(jnp.arange(half_dim, dtype=F32) * 2.0 / head_dim))
    angles = positions.astype(F32)[None, :] * inv_freq[:, None]
    return jnp.cos(angles), jnp.sin(angles)


class Place:
    def __init__(self):
        self.seq = lax.axis_index('seq')
        self.head = lax.axis_index('head')
        self.xyz = (self.seq % 4, (self.seq // 4) % 4, self.seq // 16)
        self.mem = tuple(c // 2 for c in self.xyz)
        self.cls = tuple(((c + 1) // 2) % 2 for c in self.xyz)
        self.core = (self.mem[0] + self.mem[1]) % 2
        self.kv_local = 2 * self.mem[1] + self.mem[0]
        self.member = 2 * self.mem[2] + self.mem[1]
        same_z = 1 - lax.rem(self.head + self.mem[2], 2)
        self.flag = same_z * (1 - lax.rem(self.head + self.core, 2))

    def at(self, mem):
        cs = [m * 3 + c * (1 - 2 * m) for m, c in zip(mem, self.cls)]
        return cs[2] * 16 + cs[1] * 4 + cs[0]

    def target(self, t):
        return self.at((t % 2, t // 2, self.head))

    def source_mem(self, i):
        my = i % 2
        return ((my + self.head) % 2, my, i // 2)

    def source(self, i):
        return self.at(self.source_mem(i))

    def steps(self, i, mem):
        d = [(1 - 2 * c) * (1 - 2 * m) * s for c, m, s in zip(self.cls, mem, STRIDE)]
        turns = [d[k:] + d[:k] for k in range(3)]
        first, other = ((0, 1), (2, 0), (1, 1), (2, 2))[i]
        return [a * (1 - self.head) + b * self.head for a, b in zip(turns[first], turns[other])]

    def across(self, i, crossed):
        steps = self.steps(i, self.source_mem(i))
        return functools.reduce(lambda a, d: a + steps[d], crossed, self.source(i))

    def second(self, t):
        mem = (t % 2, t // 2, self.head)
        d = [(1 - 2 * c) * (1 - 2 * m) * s for c, m, s in zip(self.cls, mem, STRIDE)]
        low = d[0] * (1 - self.core) + d[1] * self.core
        high = d[2] * (1 - self.core) + d[0] * self.core
        return self.at(mem) + low * (1 - self.mem[1]) + high * self.mem[1]

    def s_self(self, i):
        return self.flag * (1 - lax.rem(i // 2 + self.mem[2], 2)) * (1 - lax.rem(i % 2 + self.mem[1], 2))

    def t_self(self, t):
        return self.flag * (1 - lax.rem(t // 2 + self.mem[1], 2)) * (1 - lax.rem(t % 2 + self.mem[0], 2))


def fold_max(x):
    return jnp.max(x.reshape(x.shape[0] // RC, RC, x.shape[1]), axis=0)


def fold_sum(x):
    return jnp.sum(x.reshape(x.shape[0] // RC, RC, x.shape[1]), axis=0)


def attn_logits(first, c, kv_all, qa, qb, sbuf, off, mx_ref, moff):
    cols = pl.ds(c * TOK, TOK)
    keys = kv_all[pl.ds(first, NB), 0:LN, :].reshape(HALF, LN)
    sa = jnp.dot(keys, qa[:, cols], preferred_element_type=F32) * (LOG2E / 8.0)
    sb = jnp.dot(keys, qb[:, cols], preferred_element_type=F32) * (LOG2E / 8.0)
    sbuf[pl.ds(off, HALF), cols] = sa
    sbuf[pl.ds(off + HALF, HALF), cols] = sb
    mx_ref[pl.ds(moff, RC), cols] = jnp.maximum(fold_max(sa), fold_max(sb))


def attn_update(cols, mx, parts, vTs, m_ref, l_ref, acc_ref):
    m_old = m_ref[0:1, cols]
    m_new = jnp.maximum(m_old, jnp.max(mx, axis=0, keepdims=True))
    alpha = jnp.exp2(m_old - m_new)
    m_ref[:, cols] = jnp.broadcast_to(m_new, (8, TOK))
    lsum = l_ref[:, cols] * alpha
    ps = []
    for s in parts:
        p = jnp.exp2(s - m_new)
        lsum = lsum + fold_sum(p)
        ps.append(p.astype(BF16))
    l_ref[:, cols] = lsum
    pv = jnp.dot(jnp.concatenate(vTs, axis=1), jnp.concatenate(ps, axis=0), preferred_element_type=F32)
    acc_ref[:, cols] = acc_ref[:, cols] * alpha + pv


def values_of(kv_all, first, blocks):
    return [kv_all[first + b, LN + HD * h:192 + HD * h, :] for h in range(2) for b in range(blocks)]


def attn_tail(first, t, kv_all, sbuf, off, m_ref, l_ref, acc_ref):
    for c in FOUR:
        cols = pl.ds(c * TOK, TOK)
        ti = lax.broadcasted_iota(jnp.int32, (LN, TOK), 1)
        ki = lax.broadcasted_iota(jnp.int32, (LN, TOK), 0)
        parts = []
        for h in range(2):
            base = pl.multiple_of(off + h * HALF, LN)
            if t > 0:
                parts.append(sbuf[pl.ds(base, t * LN), cols])
            parts.append(jnp.where(ki + h * LN <= ti, sbuf[pl.ds(base + t * LN, LN), cols], NEG))
        mx = functools.reduce(jnp.maximum, [fold_max(p) for p in parts])
        attn_update(cols, mx, parts, values_of(kv_all, first, t + 1), m_ref, l_ref, acc_ref)


def attn_start(i, qT, state):
    qa, qb, m_ref, l_ref, acc_ref, _, _ = state
    zero = jnp.zeros((HD, TOK), BF16)
    for g in FOUR:
        q = qT[g * HD:(g + 1) * HD, :]
        cols = pl.ds(g * TOK, TOK)
        qa[i, :, cols] = jnp.concatenate([q, zero], axis=0)
        qb[i, :, cols] = jnp.concatenate([zero, q], axis=0)
    m_ref[i] = jnp.full((8, QW), NEG, F32)
    l_ref[i] = jnp.zeros((RC, QW), F32)
    acc_ref[i] = jnp.zeros((HD, QW), F32)


def attn_step(now, then, p, kv, state):
    qa, qb, m_ref, l_ref, acc_ref, sbuf, mx_ref = state
    i, group = now
    j, after = then
    for c in FOUR:
        attn_logits(after * NB, c, kv, qa.at[j], qb.at[j], sbuf, (1 - p) * TK, mx_ref, (1 - p) * RC)
        cols = pl.ds(c * TOK, TOK)
        attn_update(cols, mx_ref[pl.ds(p * RC, RC), cols], [sbuf[pl.ds(p * TK, TK), cols]], values_of(kv, group * NB, NB), m_ref.at[i], l_ref.at[i], acc_ref.at[i])


def attn_prime(i, group, kv, state):
    qa, qb, _, _, _, sbuf, mx_ref = state
    for c in FOUR:
        attn_logits(group * NB, c, kv, qa.at[i], qb.at[i], sbuf, 0, mx_ref, 0)


def attn_early(part, kv, state):
    def at(s):
        last = s // 8
        more = 1 - last * part
        return (2 + s // 4 - last) * more, ((s % 4) // 2 * 4 + 2 * part + s % 2) * more

    attn_prime(2, 2 * part, kv, state)

    def turn(n, carry):
        for e in FOUR:
            attn_step(at(4 * n + e), at(4 * n + e + 1), e % 2, kv, state)
        return carry

    lax.fori_loop(0, 2, turn, 0)


def attn_block(i, pos, kv, state):
    qa, qb, m_ref, l_ref, acc_ref, sbuf, mx_ref = state
    first = i // 2 * 8
    groups = pos // NB - first

    @pl.when(i > 0)
    def _():
        attn_prime(i, first, kv, state)

    def one(n, p):
        attn_step((i, first + n), (i, first + n + 1), p, kv, state)

    done = groups // 4 * 4

    @pl.when(groups >= 4)
    def _():
        for n in FOUR:
            one(n, n % 2)

    @pl.when(groups - done >= 2)
    def _():
        one(done, 0)
        one(done + 1, 1)

    @pl.when(groups % 2 == 1)
    def _():
        one(groups - 1, 0)
    for t in range(NB):
        @pl.when(pos % NB == t)
        def _():
            attn_tail(pos // NB * NB, t, kv, sbuf, (groups % 2) * TK, m_ref.at[i], l_ref.at[i], acc_ref.at[i])
    oT = acc_ref[i] / jnp.sum(l_ref[i], axis=0, keepdims=True)
    halves = []
    for g in range(0, 4, 2):
        two = jnp.concatenate([oT[:, g * TOK:(g + 1) * TOK], oT[:, (g + 1) * TOK:(g + 2) * TOK]], axis=0)
        halves.append(two.T.astype(BF16))
    return jnp.concatenate(halves, axis=1)


def stack_kernel(x_hbm, gain_ref, cos_hbm, sin_hbm, wq, wk, wv, wg, wu, wd, wo, x_ref, k_ref, v_ref,
                 cosT, sinT, h_ref, q_send, kv_send, q_all, kv_all, o_send, o_full, mlp, part_in, hid, wqb, wkvb, wgb, wub, wdb, wob,
                 qa, qb, m_ref, l_ref, acc_ref, sbuf, mx_ref,
                 xsem, wsem, msem, osem, skv, sq, sag, sdd, so, sp, rkv, rq, rag, rdd, ro, rp):
    me = Place()
    sib = 1 - me.head
    state = (qa, qb, m_ref, l_ref, acc_ref, sbuf, mx_ref)

    def remote(src, dst, ssem, rsem, seq, head):
        return pltpu.make_async_remote_copy(src_ref=src, dst_ref=dst, send_sem=ssem, recv_sem=rsem, device_id={'seq': seq, 'head': head}, device_id_type=MESH)

    def for_others(is_self, fn):
        for i in FOUR:
            @pl.when(is_self(i) == 0)
            def _():
                fn(i)

    start_cps = [pltpu.make_async_copy(x_hbm, x_ref, xsem.at[0]), pltpu.make_async_copy(cos_hbm, cosT, xsem.at[1]), pltpu.make_async_copy(sin_hbm, sinT, xsem.at[2])]

    def proj_copies(layer):
        return (pltpu.make_async_copy(wk.at[layer], wkvb.at[pl.ds(0, TOK)], wsem.at[0]), pltpu.make_async_copy(wv.at[layer], wkvb.at[pl.ds(TOK, TOK)], wsem.at[1]), pltpu.make_async_copy(wq.at[layer], wqb, wsem.at[2]))

    for c in start_cps:
        c.start()
    for n in range(2):
        proj_copies(0)[n].start()

    barrier = pltpu.get_barrier_semaphore()

    def hello(seq, head):
        pl.semaphore_signal(barrier, inc=1, device_id={'seq': seq, 'head': head}, device_id_type=MESH)

    for_others(me.s_self, lambda i: hello(me.source(i), me.mem[2]))
    for_others(me.t_self, lambda t: hello(me.target(t), me.core))
    for i in range(2):
        hello(me.across(i, (0,)), me.mem[2])
    for step in me.steps(0, me.mem):
        hello(me.seq + step, me.head)
    hello(me.seq, sib)

    def gu_copies(layer, n):
        off = pl.multiple_of(n * TOK, TOK)
        slot = n % 3
        return (pltpu.make_async_copy(wg.at[layer, :, pl.ds(off, TOK)], wgb.at[slot], msem.at[0, slot]), pltpu.make_async_copy(wu.at[layer, :, pl.ds(off, TOK)], wub.at[slot], msem.at[1, slot]))

    def d_copy(layer, n):
        return pltpu.make_async_copy(wd.at[layer, pl.ds(pl.multiple_of(n * TOK, TOK), TOK)], wdb.at[n % 3], msem.at[2, n % 3])

    def first_tiles(layer):
        for n in range(3):
            for c in gu_copies(layer, n):
                c.start()
        for n in range(2):
            d_copy(layer, n).start()

    for c in start_cps:
        c.wait()
    proj_copies(0)[2].start()

    def rope(a):
        lo, hi = a[0:32], a[32:HD]
        return jnp.concatenate([lo * cosT[:] - hi * sinT[:], hi * cosT[:] + lo * sinT[:]], axis=0)

    def project(w):
        return lax.dot_general(w, h_ref[:], NT, preferred_element_type=F32).astype(BF16)

    def layer_body(layer, carry):
        kv = kv_all.at[layer]
        xf = x_ref[:].astype(F32)
        inv = lax.rsqrt(jnp.mean(xf * xf, axis=-1, keepdims=True) + EPS)
        gain = jnp.where(layer == 0, gain_ref[0:1, :].astype(F32), gain_ref[1:2, :].astype(F32))
        h_ref[:] = (xf * inv * gain).astype(BF16)

        w_cps = proj_copies(layer)
        w_cps[0].wait()
        w_cps[1].wait()
        kvT = project(wkvb[:])
        for t in FOUR:
            k = rope(kvT[t * HD:(t + 1) * HD].astype(F32)).astype(BF16)
            k_ref[layer, t * HD:(t + 1) * HD, :] = k
            kf = k.astype(F32)
            kv_send[layer, t, 0:LN, :] = jnp.concatenate([kf[:, :LN], kf[:, LN:TOK]], axis=0).T.astype(BF16)
            v = kvT[TOK + t * HD:TOK + (t + 1) * HD]
            v_ref[layer, t * HD:(t + 1) * HD, :] = v
            kv_send[layer, t, LN:LN + HD, :] = v[:, :LN]
            kv_send[layer, t, LN + HD:TOK, :] = v[:, LN:TOK]

        @pl.when(layer == 0)
        def _():
            first_tiles(0)

        @pl.when(layer == 0)
        def _():
            pl.semaphore_wait(barrier, 12 - 2 * me.flag + 4 * (1 - me.mem[2]))

        def kv_copy(t):
            return remote(kv_send.at[layer, t], kv.at[me.seq], skv.at[layer, t], rkv.at[layer, me.member], me.target(t), me.core)

        def q_copy(t):
            return remote(q_send.at[layer, t], q_all.at[layer, me.member], sq.at[layer, t], rq.at[layer, me.member], me.target(t), me.core)

        def second_copy(t):
            return remote(kv_send.at[layer, t], kv.at[me.seq], skv.at[layer, 4 + t], rag.at[layer, me.mem[1], 0], me.second(t), me.core)

        for_others(me.t_self, lambda t: kv_copy(t).start())

        @pl.when(me.mem[2] == 0)
        def _():
            for t in FOUR:
                second_copy(t).start()
        for t in FOUR:
            @pl.when(me.t_self(t) == 1)
            def _():
                kv[me.seq] = kv_send[layer, t]

        w_cps[2].wait()
        for t in FOUR:
            qT = project(wqb[t * TOK:(t + 1) * TOK])
            for g in FOUR:
                q_send[layer, t, g * HD:(g + 1) * HD, :] = rope(qT[g * HD:(g + 1) * HD].astype(F32)).astype(BF16)

        def send_queries():
            for_others(me.t_self, lambda t: q_copy(t).start())
            for t in FOUR:
                @pl.when(me.t_self(t) == 1)
                def _():
                    q_all[layer, me.member] = q_send[layer, t]

        def ag(i, k):
            dim, crossed = SENDS[k]
            block = kv.at[me.across(i, crossed)]
            return remote(block, block, sag.at[layer], rag.at[layer, i, k], me.seq + me.steps(i, me.mem)[dim], me.head)

        def relay(i, crossed):
            block = kv.at[me.across(i, crossed)]
            remote(block, block, sdd.at[layer], rdd.at[layer, min(i, 2)], me.seq, sib).start()

        def arrived(i, k):
            dim, crossed = SENDS[k]
            block = kv.at[me.across(i, crossed + (dim,))]
            remote(block, block, sag.at[layer], rag.at[layer, i, k], me.seq, sib).wait_recv()

        def step(part, number):
            members = PARTS[part]
            if number == 0:
                for i in members:
                    @pl.when(me.s_self(i) == 0)
                    def _():
                        remote(kv_send.at[layer, 0], kv.at[me.source(i)], skv.at[layer, 0], rkv.at[layer, i], me.seq, sib).wait_recv()
                for k in ((1, 3) if part < 2 else (0, 1, 3)):
                    for i in members:
                        ag(i, k).start()
                for i in members:
                    relay(i, ())
            first = (0,) if number == (part == 2) else ()
            waits = first if number < 2 else SECOND if number == 2 else THIRD
            for k in waits:
                for i in members:
                    arrived(i, k)
                    for nxt in NEXT[k]:
                        ag(i, nxt).start()
            for k in waits:
                for i in members:
                    relay(i, SENDS[k][1] + (SENDS[k][0],))

        def from_sibling(part):
            blocks = kv.at[pl.ds(0, 8 * len(PARTS[part]))]
            remote(blocks, blocks, sdd.at[layer], rdd.at[layer, part], me.seq, sib).wait_recv()

        def gate_up(n):
            g = jnp.dot(h_ref[:], wgb[n % 3], preferred_element_type=F32)
            u = jnp.dot(h_ref[:], wub[n % 3], preferred_element_type=F32)
            return (g * jax.nn.sigmoid(g) * u).astype(BF16)

        def add_down(hidden, n):
            d = jnp.dot(hidden, wdb[n % 3], preferred_element_type=F32)
            for c in range(8):
                part = d[:, c * TOK:(c + 1) * TOK]
                mlp[layer, c] = part if n == 0 else mlp[layer, c] + part

        for c in gu_copies(layer, 0):
            c.wait()
        hid[:] = gate_up(0)
        for c in gu_copies(layer, 3):
            c.start()
        d_copy(layer, 2).start()

        def tile(n):
            for c in gu_copies(layer, n):
                c.wait()
            d_copy(layer, n - 1).wait()
            before = hid[:]
            now = gate_up(n)
            add_down(before, n - 1)
            hid[:] = now
            if n + 3 < N_TILES:
                for c in gu_copies(layer, n + 3):
                    c.start()
            if n + 2 < N_TILES:
                d_copy(layer, n + 2).start()

        for n in range(1, BEFORE):
            for part, number in EVENTS.get(n, ()):
                step(part, number)
            if n == 7:
                send_queries()
            tile(n)

        o_cp = pltpu.make_async_copy(wo.at[layer], wob, osem.at[0])
        o_cp.start()

        @pl.when(layer == 0)
        def _():
            for c in proj_copies(1):
                c.start()
        for part, number in EVENTS[BEFORE]:
            step(part, number)
        for_others(me.s_self, lambda i: remote(q_send.at[layer, 0], q_all.at[layer, i], sq.at[layer, 0], rq.at[layer, i], me.seq, sib).wait_recv())
        from_sibling(0)

        def o_copy(i):
            return remote(o_send.at[layer, i], o_full.at[layer, me.kv_local], so.at[layer, i], ro.at[layer, me.kv_local], me.source(i), me.mem[2])

        lax.fori_loop(0, 4, lambda i, carry: attn_start(i, q_all[layer, i], state) or carry, 0)
        def early(part, carry):
            attn_early(part, kv, state)
            @pl.when(part == 0)
            def _():
                for which, number in EVENTS[N_TILES]:
                    step(which, number)
                from_sibling(1)

            @pl.when(part == 1)
            def _():
                for which, number in EVENTS[N_TILES + 1]:
                    step(which, number)
            return carry

        lax.fori_loop(0, 2, early, 0)

        def query(i, carry):
            @pl.when(i == 2)
            def _():
                from_sibling(2)

            o_send[layer, i] = attn_block(i, me.source(i), kv, state)

            @pl.when(me.s_self(i) == 0)
            def _():
                o_copy(i).start()

            @pl.when(me.s_self(i) == 1)
            def _():
                o_full[layer, me.kv_local] = o_send[layer, i]
            return carry

        lax.fori_loop(0, 4, query, 0)
        for n in range(BEFORE, N_TILES):
            tile(n)
        d_copy(layer, N_TILES - 1).wait()
        add_down(hid[:], N_TILES - 1)

        @pl.when(layer == 0)
        def _():
            first_tiles(1)

        o_cp.wait()
        for_others(me.t_self, lambda t: remote(o_send.at[layer, 0], o_full.at[layer, t], so.at[layer, 0], ro.at[layer, t], me.seq, sib).wait_recv())

        def p_copy(n):
            return remote(mlp.at[layer, n], part_in.at[layer, n], sp.at[layer], rp.at[layer, n], me.seq, sib)

        heads = jnp.concatenate([o_full[layer, t] for t in FOUR], axis=1)
        for n in range(0, 8, 2):
            d = jnp.dot(heads, wob[:, n * TOK:(n + 2) * TOK], preferred_element_type=F32)
            for e in range(2):
                mlp[layer, n + e] += d[:, e * TOK:(e + 1) * TOK]
                p_copy(n + e).start()
        for n in range(8):
            cols = pl.ds(n * TOK, TOK)
            p_copy(n).wait_recv()
            y = (mlp[layer, n] + part_in[layer, n]).astype(BF16)
            x_ref[:, cols] = (x_ref[:, cols].astype(F32) + y.astype(F32)).astype(BF16)
        return carry

    lax.fori_loop(0, 2, layer_body, 0)

    def drain(layer, carry):
        def gone(src, sem):
            remote(src, src, sem, rp.at[layer, 0], me.seq, sib).wait_send()

        for_others(me.t_self, lambda t: gone(kv_send.at[layer, t], skv.at[layer, t]))
        for_others(me.t_self, lambda t: gone(q_send.at[layer, t], sq.at[layer, t]))
        for_others(me.s_self, lambda i: gone(o_send.at[layer, i], so.at[layer, i]))
        gone(kv_all.at[layer, pl.ds(0, 26)], sag.at[layer])

        @pl.when(me.mem[2] == 0)
        def _():
            for t in FOUR:
                gone(kv_send.at[layer, t], skv.at[layer, 4 + t])
        gone(kv_all.at[layer, pl.ds(0, 32)], sdd.at[layer])
        gone(mlp.at[layer], sp.at[layer])
        return carry

    lax.fori_loop(0, 2, drain, 0)


def finish_kernel(x_in, k_in, v_in, x_out, k_out, v_out, sem):
    cps = [pltpu.make_async_copy(a, b, sem.at[n]) for n, (a, b) in enumerate(((x_in, x_out), (k_in, k_out), (v_in, v_out)))]
    for c in cps:
        c.start()
    for c in cps:
        c.wait()


def vmem(*shape, dtype=BF16):
    return pltpu.VMEM(shape, dtype)


BEFORE = 15
EVENTS = {5: ((0, 0),), 6: ((1, 0),), 9: ((0, 2),), 10: ((1, 2),), 12: ((2, 0),), 13: ((0, 4),), 15: ((1, 4), (2, 1)), 16: ((2, 2),), 17: ((2, 4),)}


SCRATCH = [
    vmem(32, TOK, dtype=F32), vmem(32, TOK, dtype=F32), vmem(TOK, DM), vmem(2, 4, TOK, TOK), vmem(2, 4, TOK, LN), vmem(2, 4, TOK, TOK), vmem(2, HD, TOK, LN),
    vmem(2, 4, TOK, TOK), vmem(2, 4, TOK, TOK), vmem(2, 8, TOK, TOK, dtype=F32), vmem(2, 8, TOK, TOK, dtype=F32), vmem(TOK, TOK),
    vmem(QW, DM), vmem(2 * TOK, DM), vmem(3, DM, TOK), vmem(3, DM, TOK), vmem(3, TOK, DM), vmem(QW, DM),
    vmem(4, LN, QW), vmem(4, LN, QW), vmem(4, 8, QW, dtype=F32), vmem(4, RC, QW, dtype=F32), vmem(4, HD, QW, dtype=F32), vmem(2 * TK, QW, dtype=F32), vmem(2 * RC, QW, dtype=F32),
] + [pltpu.SemaphoreType.DMA(s) for s in ((3,), (3,), (3, 3), (1,), (2, 8), (2, 4), (2,), (2,), (2, 4), (2,), (2, 4), (2, 4), (2, 4, 7), (2, 3), (2, 4), (2, 8))]


def solution(mesh):
    row_spec = P(('batch', 'seq'), None)
    pos_spec = P(('batch', 'seq'))
    head_spec = P(None, None, 'head', None)
    out_proj_spec = P(None, 'head', None, None)
    col_spec = P(None, None, 'head')
    down_spec = P(None, 'head', None)
    cache_spec = P(None, ('batch', 'seq'), 'head', None)
    in_vmem = pl.BlockSpec(memory_space=pltpu.VMEM)
    anywhere = pl.BlockSpec(memory_space=pl.ANY)

    def local_forward(x, pos, w_q, w_k, w_v, w_o, w_gate, w_up, w_down, gain):
        cosT, sinT = rope_tables(pos, HD)
        wq = w_q.transpose(0, 2, 3, 1).reshape(2, QW, DM)
        wk = w_k.transpose(0, 2, 3, 1).reshape(2, TOK, DM)
        wv = w_v.transpose(0, 2, 3, 1).reshape(2, TOK, DM)
        wo = w_o.reshape(2, QW, DM)
        x, kT, vT = pl.pallas_call(
            stack_kernel,
            out_shape=tuple(pltpu.VMEM(s, BF16) for s in OUT_SHAPES),
            in_specs=[anywhere, in_vmem] + [anywhere] * 9,
            out_specs=(in_vmem,) * 3,
            scratch_shapes=SCRATCH,
            compiler_params=pltpu.CompilerParams(collective_id=0, has_side_effects=True, vmem_limit_bytes=VMEM_LIMIT),
            name='stack',
        )(x, gain, cosT, sinT, wq, wk, wv, w_gate, w_up, w_down, wo)
        x, kT, vT = pl.pallas_call(
            finish_kernel,
            out_shape=tuple(jax.ShapeDtypeStruct(s, BF16) for s in OUT_SHAPES),
            in_specs=[in_vmem] * 3,
            out_specs=(anywhere,) * 3,
            scratch_shapes=[pltpu.SemaphoreType.DMA((3,))],
            compiler_params=pltpu.CompilerParams(vmem_limit_bytes=QW * QW),
            name='finish',
        )(*[pltpu.with_memory_space_constraint(a, pltpu.VMEM) for a in (x, kT, vT)])
        k_cache = kT.reshape(2, 4, HD, TOK).transpose(0, 3, 1, 2)
        v_cache = vT.reshape(2, 4, HD, TOK).transpose(0, 3, 1, 2)
        return x, k_cache, v_cache

    return jax.shard_map(local_forward, mesh=mesh, in_specs=(row_spec, pos_spec, head_spec, head_spec, head_spec, out_proj_spec, col_spec, col_spec, down_spec, P(None, None)), out_specs=(row_spec, cache_spec, cache_spec), check_vma=False)


OUT_SHAPES = ((TOK, DM), (2, TOK, TOK), (2, TOK, TOK))
```

```python
import functools
import jax
import jax.numpy as jnp
from jax import lax
from jax.experimental import pallas as pl
from jax.experimental.pallas import tpu as pltpu
from jax.sharding import PartitionSpec as P

ROPE_BASE = 500000.0
EPS = 1e-5
LOG2E = 1.4426950408889634
NEG = -1e30
MESH = pl.DeviceIdType.MESH
TOK, DM, QW, LN, HD = 256, 2048, 1024, 128, 64
F32 = jnp.float32
BF16 = jnp.bfloat16
VMEM_LIMIT = 62 * 1024 * 1024

STRIDE = (1, 4, 16)
N_TILES = 16
NB = 4
TK = NB * TOK
HALF = NB * LN
RC = 8
NT = (((1,), (1,)), ((), ()))
PARTS = ((0,), (1,), (2, 3))
SENDS = ((0, ()), (1, ()), (1, (0,)), (2, ()), (2, (0,)), (2, (1,)), (2, (0, 1)))
SECOND, THIRD = (1, 2), (3, 4, 5, 6)
NEXT = ((2, 4), (5,), (6,), (), (), (), ())
FOUR = range(4)


class Place:
    def __init__(self):
        self.seq = lax.axis_index('seq')
        self.head = lax.axis_index('head')
        self.xyz = (self.seq % 4, (self.seq // 4) % 4, self.seq // 16)
        self.mem = tuple(c // 2 for c in self.xyz)
        self.cls = tuple(((c + 1) // 2) % 2 for c in self.xyz)
        self.core = (self.mem[0] + self.mem[1]) % 2
        self.kv_local = 2 * self.mem[1] + self.mem[0]
        self.member = 2 * self.mem[2] + self.mem[1]
        same_z = 1 - lax.rem(self.head + self.mem[2], 2)
        self.flag = same_z * (1 - lax.rem(self.head + self.core, 2))

    def at(self, mem):
        cs = [m * 3 + c * (1 - 2 * m) for m, c in zip(mem, self.cls)]
        return cs[2] * 16 + cs[1] * 4 + cs[0]

    def target(self, t):
        return self.at((t % 2, t // 2, self.head))

    def source_mem(self, i):
        my = i % 2
        return ((my + self.head) % 2, my, i // 2)

    def source(self, i):
        return self.at(self.source_mem(i))

    def steps(self, i, mem):
        d = [(1 - 2 * c) * (1 - 2 * m) * s for c, m, s in zip(self.cls, mem, STRIDE)]
        turns = [d[k:] + d[:k] for k in range(3)]
        first, other = ((0, 1), (2, 0), (1, 1), (2, 2))[i]
        return [a * (1 - self.head) + b * self.head for a, b in zip(turns[first], turns[other])]

    def across(self, i, crossed):
        steps = self.steps(i, self.source_mem(i))
        return functools.reduce(lambda a, d: a + steps[d], crossed, self.source(i))

    def second(self, t):
        mem = (t % 2, t // 2, self.head)
        d = [(1 - 2 * c) * (1 - 2 * m) * s for c, m, s in zip(self.cls, mem, STRIDE)]
        low = d[0] * (1 - self.core) + d[1] * self.core
        high = d[2] * (1 - self.core) + d[0] * self.core
        return self.at(mem) + low * (1 - self.mem[1]) + high * self.mem[1]

    def s_self(self, i):
        return self.flag * (1 - lax.rem(i // 2 + self.mem[2], 2)) * (1 - lax.rem(i % 2 + self.mem[1], 2))

    def t_self(self, t):
        return self.flag * (1 - lax.rem(t // 2 + self.mem[1], 2)) * (1 - lax.rem(t % 2 + self.mem[0], 2))


def fold_max(x):
    return jnp.max(x.reshape(x.shape[0] // RC, RC, x.shape[1]), axis=0)


def fold_sum(x):
    return jnp.sum(x.reshape(x.shape[0] // RC, RC, x.shape[1]), axis=0)


def attn_logits(first, c, kv_all, qa, qb, sbuf, off, mx_ref, moff):
    cols = pl.ds(c * TOK, TOK)
    keys = kv_all[pl.ds(first, NB), 0:LN, :].reshape(HALF, LN)
    sa = jnp.dot(keys, qa[:, cols], preferred_element_type=F32) * (LOG2E / 8.0)
    sb = jnp.dot(keys, qb[:, cols], preferred_element_type=F32) * (LOG2E / 8.0)
    sbuf[pl.ds(off, HALF), cols] = sa
    sbuf[pl.ds(off + HALF, HALF), cols] = sb
    mx_ref[pl.ds(moff, RC), cols] = jnp.maximum(fold_max(sa), fold_max(sb))


def attn_update(cols, mx, parts, vTs, m_ref, l_ref, acc_ref):
    m_old = m_ref[0:1, cols]
    m_new = jnp.maximum(m_old, jnp.max(mx, axis=0, keepdims=True))
    alpha = jnp.exp2(m_old - m_new)
    m_ref[:, cols] = jnp.broadcast_to(m_new, (8, TOK))
    lsum = l_ref[:, cols] * alpha
    ps = []
    for s in parts:
        p = jnp.exp2(s - m_new)
        lsum = lsum + fold_sum(p)
        ps.append(p.astype(BF16))
    l_ref[:, cols] = lsum
    pv = jnp.dot(jnp.concatenate(vTs, axis=1), jnp.concatenate(ps, axis=0), preferred_element_type=F32)
    acc_ref[:, cols] = acc_ref[:, cols] * alpha + pv


def values_of(kv_all, first, blocks):
    return [kv_all[first + b, LN + HD * h:192 + HD * h, :] for h in range(2) for b in range(blocks)]


def attn_tail(first, t, kv_all, sbuf, off, m_ref, l_ref, acc_ref):
    for c in FOUR:
        cols = pl.ds(c * TOK, TOK)
        ti = lax.broadcasted_iota(jnp.int32, (LN, TOK), 1)
        ki = lax.broadcasted_iota(jnp.int32, (LN, TOK), 0)
        parts = []
        for h in range(2):
            base = pl.multiple_of(off + h * HALF, LN)
            if t > 0:
                parts.append(sbuf[pl.ds(base, t * LN), cols])
            parts.append(jnp.where(ki + h * LN <= ti, sbuf[pl.ds(base + t * LN, LN), cols], NEG))
        mx = functools.reduce(jnp.maximum, [fold_max(p) for p in parts])
        attn_update(cols, mx, parts, values_of(kv_all, first, t + 1), m_ref, l_ref, acc_ref)


def attn_start(i, qT, state):
    qa, qb, m_ref, l_ref, acc_ref, _, _ = state
    zero = jnp.zeros((HD, TOK), BF16)
    for g in FOUR:
        q = qT[g * HD:(g + 1) * HD, :]
        cols = pl.ds(g * TOK, TOK)
        qa[i, :, cols] = jnp.concatenate([q, zero], axis=0)
        qb[i, :, cols] = jnp.concatenate([zero, q], axis=0)
    m_ref[i] = jnp.full((8, QW), NEG, F32)
    l_ref[i] = jnp.zeros((RC, QW), F32)
    acc_ref[i] = jnp.zeros((HD, QW), F32)


def attn_step(now, then, p, kv, state):
    qa, qb, m_ref, l_ref, acc_ref, sbuf, mx_ref = state
    i, group = now
    j, after = then
    for c in FOUR:
        attn_logits(after * NB, c, kv, qa.at[j], qb.at[j], sbuf, (1 - p) * TK, mx_ref, (1 - p) * RC)
        cols = pl.ds(c * TOK, TOK)
        attn_update(cols, mx_ref[pl.ds(p * RC, RC), cols], [sbuf[pl.ds(p * TK, TK), cols]], values_of(kv, group * NB, NB), m_ref.at[i], l_ref.at[i], acc_ref.at[i])


def attn_prime(i, group, kv, state):
    qa, qb, _, _, _, sbuf, mx_ref = state
    for c in FOUR:
        attn_logits(group * NB, c, kv, qa.at[i], qb.at[i], sbuf, 0, mx_ref, 0)


def attn_early(n, kv, state):
    def at(s):
        s = 4 * n + s
        more = 1 - s // 16
        return (2 + s // 4 % 2) * more, ((s % 4) // 2 * 4 + 2 * (s // 8) + s % 2) * more

    @pl.when(n % 2 == 0)
    def _():
        attn_prime(2, n, kv, state)
    for e in FOUR:
        ahead = at(e + 1) if e < 3 else tuple(jnp.where(n == 1, a, b) for a, b in zip(at(e), at(e + 1)))
        attn_step(at(e), ahead, e % 2, kv, state)


def attn_block(i, pos, kv, state):
    qa, qb, m_ref, l_ref, acc_ref, sbuf, mx_ref = state
    first = i // 2 * 8
    groups = pos // NB - first

    @pl.when(i > 0)
    def _():
        attn_prime(i, first, kv, state)

    def one(n, p):
        attn_step((i, first + n), (i, first + n + 1), p, kv, state)

    done = groups // 4 * 4

    @pl.when(groups >= 4)
    def _():
        for n in FOUR:
            one(n, n % 2)

    @pl.when(groups - done >= 2)
    def _():
        one(done, 0)
        one(done + 1, 1)

    @pl.when(groups % 2 == 1)
    def _():
        one(groups - 1, 0)
    for t in range(NB):
        @pl.when(pos % NB == t)
        def _():
            attn_tail(pos // NB * NB, t, kv, sbuf, (groups % 2) * TK, m_ref.at[i], l_ref.at[i], acc_ref.at[i])
    oT = acc_ref[i] / jnp.sum(l_ref[i], axis=0, keepdims=True)
    halves = []
    for g in range(0, 4, 2):
        two = jnp.concatenate([oT[:, g * TOK:(g + 1) * TOK], oT[:, (g + 1) * TOK:(g + 2) * TOK]], axis=0)
        halves.append(two.T.astype(BF16))
    return jnp.concatenate(halves, axis=1)


def stack_kernel(x_hbm, gain_ref, pos_ref, wq, wk, wv, wg, wu, wd, wo, x_ref, k_ref, v_ref,
                 cosT, sinT, h_ref, q_send, kv_send, q_all, kv_all, o_send, o_full, mlp, part_in, hid, wqb, wkvb, wgb, wub, wdb, wob,
                 qa, qb, m_ref, l_ref, acc_ref, sbuf, mx_ref,
                 xsem, wsem, msem, osem, skv, sq, sag, sdd, so, sp, rkv, rq, rag, rdd, ro, rp):
    me = Place()
    sib = 1 - me.head
    state = (qa, qb, m_ref, l_ref, acc_ref, sbuf, mx_ref)

    def remote(src, dst, ssem, rsem, seq, head):
        return pltpu.make_async_remote_copy(src_ref=src, dst_ref=dst, send_sem=ssem, recv_sem=rsem, device_id={'seq': seq, 'head': head}, device_id_type=MESH)

    def for_others(is_self, fn):
        for i in FOUR:
            @pl.when(is_self(i) == 0)
            def _():
                fn(i)

    start_cps = [pltpu.make_async_copy(x_hbm, x_ref, xsem.at[0])]

    def proj_copies(layer):
        return (pltpu.make_async_copy(wk.at[layer], wkvb.at[pl.ds(0, TOK)], wsem.at[0]), pltpu.make_async_copy(wv.at[layer], wkvb.at[pl.ds(TOK, TOK)], wsem.at[1]), pltpu.make_async_copy(wq.at[layer], wqb, wsem.at[2]))

    for c in start_cps:
        c.start()
    for n in range(2):
        proj_copies(0)[n].start()

    barrier = pltpu.get_barrier_semaphore()

    def hello(seq, head):
        pl.semaphore_signal(barrier, inc=1, device_id={'seq': seq, 'head': head}, device_id_type=MESH)

    for_others(me.s_self, lambda i: hello(me.source(i), me.mem[2]))
    for_others(me.t_self, lambda t: hello(me.target(t), me.core))
    for i in range(2):
        hello(me.across(i, (0,)), me.mem[2])
    for step in me.steps(0, me.mem):
        hello(me.seq + step, me.head)
    hello(me.seq, sib)

    def gu_copies(layer, n):
        off = pl.multiple_of(n * TOK, TOK)
        slot = n % 3
        return (pltpu.make_async_copy(wg.at[layer, :, pl.ds(off, TOK)], wgb.at[slot], msem.at[0, slot]), pltpu.make_async_copy(wu.at[layer, :, pl.ds(off, TOK)], wub.at[slot], msem.at[1, slot]))

    def d_copy(layer, n):
        return pltpu.make_async_copy(wd.at[layer, pl.ds(pl.multiple_of(n * TOK, TOK), TOK)], wdb.at[n % 3], msem.at[2, n % 3])

    def first_tiles(layer):
        for n in range(3):
            for c in gu_copies(layer, n):
                c.start()
        for n in range(2):
            d_copy(layer, n).start()

    freq = ROPE_BASE ** (-(lax.broadcasted_iota(jnp.int32, (HD // 2, TOK), 0).astype(F32) * 2.0 / HD))
    angles = pos_ref[:].astype(F32) * freq
    cosT[:] = jnp.cos(angles)
    sinT[:] = jnp.sin(angles)
    for c in start_cps:
        c.wait()
    proj_copies(0)[2].start()

    def rope(a):
        lo, hi = a[0:32], a[32:HD]
        return jnp.concatenate([lo * cosT[:] - hi * sinT[:], hi * cosT[:] + lo * sinT[:]], axis=0)

    def project(w):
        return lax.dot_general(w, h_ref[:], NT, preferred_element_type=F32).astype(BF16)

    def layer_body(layer, carry):
        kv = kv_all.at[layer]
        xf = x_ref[:].astype(F32)
        inv = lax.rsqrt(jnp.mean(xf * xf, axis=-1, keepdims=True) + EPS)
        gain = jnp.where(layer == 0, gain_ref[0:1, :].astype(F32), gain_ref[1:2, :].astype(F32))
        h_ref[:] = (xf * inv * gain).astype(BF16)

        w_cps = proj_copies(layer)
        w_cps[0].wait()
        w_cps[1].wait()
        kT = project(wkvb[:TOK])
        vT = project(wkvb[TOK:])
        for t in FOUR:
            k = rope(kT[t * HD:(t + 1) * HD].astype(F32)).astype(BF16)
            k_ref[layer, t * HD:(t + 1) * HD, :] = k
            kf = k.astype(F32)
            kv_send[layer, t, 0:LN, :] = jnp.concatenate([kf[:, :LN], kf[:, LN:TOK]], axis=0).T.astype(BF16)
            v = vT[t * HD:(t + 1) * HD]
            v_ref[layer, t * HD:(t + 1) * HD, :] = v
            kv_send[layer, t, LN:LN + HD, :] = v[:, :LN]
            kv_send[layer, t, LN + HD:TOK, :] = v[:, LN:TOK]

        @pl.when(layer == 0)
        def _():
            first_tiles(0)

        @pl.when(layer == 0)
        def _():
            pl.semaphore_wait(barrier, 12 - 2 * me.flag + 4 * (1 - me.mem[2]))

        def kv_copy(t):
            return remote(kv_send.at[layer, t], kv.at[me.seq], skv.at[layer, t], rkv.at[layer, me.member], me.target(t), me.core)

        def q_copy(t):
            return remote(q_send.at[layer, t], q_all.at[layer, me.member], sq.at[layer, t], rq.at[layer, me.member], me.target(t), me.core)

        def second_copy(t):
            return remote(kv_send.at[layer, t], kv.at[me.seq], skv.at[layer, 4 + t], rag.at[layer, me.mem[1], 0], me.second(t), me.core)

        for_others(me.t_self, lambda t: kv_copy(t).start())

        @pl.when(me.mem[2] == 0)
        def _():
            for t in FOUR:
                second_copy(t).start()
        for t in FOUR:
            @pl.when(me.t_self(t) == 1)
            def _():
                kv[me.seq] = kv_send[layer, t]

        w_cps[2].wait()
        for t in FOUR:
            qT = project(wqb[t * TOK:(t + 1) * TOK])
            for g in FOUR:
                q_send[layer, t, g * HD:(g + 1) * HD, :] = rope(qT[g * HD:(g + 1) * HD].astype(F32)).astype(BF16)

        def send_queries():
            for_others(me.t_self, lambda t: q_copy(t).start())
            for t in FOUR:
                @pl.when(me.t_self(t) == 1)
                def _():
                    q_all[layer, me.member] = q_send[layer, t]

        def ag(i, k):
            dim, crossed = SENDS[k]
            block = kv.at[me.across(i, crossed)]
            return remote(block, block, sag.at[layer], rag.at[layer, i, k], me.seq + me.steps(i, me.mem)[dim], me.head)

        def relay(i, crossed):
            block = kv.at[me.across(i, crossed)]
            remote(block, block, sdd.at[layer], rdd.at[layer, min(i, 2)], me.seq, sib).start()

        def arrived(i, k):
            dim, crossed = SENDS[k]
            block = kv.at[me.across(i, crossed + (dim,))]
            remote(block, block, sag.at[layer], rag.at[layer, i, k], me.seq, sib).wait_recv()

        def step(part, number):
            members = PARTS[part]
            if number == 0:
                for i in members:
                    @pl.when(me.s_self(i) == 0)
                    def _():
                        remote(kv_send.at[layer, 0], kv.at[me.source(i)], skv.at[layer, 0], rkv.at[layer, i], me.seq, sib).wait_recv()
                for k in ((1, 3) if part < 2 else (0, 1, 3)):
                    for i in members:
                        ag(i, k).start()
                for i in members:
                    relay(i, ())
            first = (0,) if number == (part == 2) else ()
            waits = first if number < 2 else SECOND if number == 2 else THIRD
            for k in waits:
                for i in members:
                    arrived(i, k)
                    for nxt in NEXT[k]:
                        ag(i, nxt).start()
            for k in waits:
                for i in members:
                    relay(i, SENDS[k][1] + (SENDS[k][0],))

        def from_sibling(part):
            blocks = kv.at[pl.ds(0, 8 * len(PARTS[part]))]
            remote(blocks, blocks, sdd.at[layer], rdd.at[layer, part], me.seq, sib).wait_recv()

        def gate_up(n):
            g = jnp.dot(h_ref[:], wgb[n % 3], preferred_element_type=F32)
            u = jnp.dot(h_ref[:], wub[n % 3], preferred_element_type=F32)
            return (g * jax.nn.sigmoid(g) * u).astype(BF16)

        def add_down(hidden, n):
            d = jnp.dot(hidden, wdb[n % 3], preferred_element_type=F32)
            for c in range(8):
                part = d[:, c * TOK:(c + 1) * TOK]
                mlp[layer, c] = part if n == 0 else mlp[layer, c] + part

        for c in gu_copies(layer, 0):
            c.wait()
        hid[:] = gate_up(0)
        for c in gu_copies(layer, 3):
            c.start()
        d_copy(layer, 2).start()

        def tile(n):
            for c in gu_copies(layer, n):
                c.wait()
            d_copy(layer, n - 1).wait()
            before = hid[:]
            now = gate_up(n)
            add_down(before, n - 1)
            hid[:] = now
            if n + 3 < N_TILES:
                for c in gu_copies(layer, n + 3):
                    c.start()
            if n + 2 < N_TILES:
                d_copy(layer, n + 2).start()

        for n in range(1, BEFORE):
            for part, number in EVENTS.get(n, ()):
                step(part, number)
            if n == 4:
                send_queries()
            tile(n)

        o_cp = pltpu.make_async_copy(wo.at[layer], wob, osem.at[0])
        o_cp.start()

        @pl.when(layer == 0)
        def _():
            for c in proj_copies(1):
                c.start()
        for part, number in EVENTS[BEFORE]:
            step(part, number)
        for_others(me.s_self, lambda i: remote(q_send.at[layer, 0], q_all.at[layer, i], sq.at[layer, 0], rq.at[layer, i], me.seq, sib).wait_recv())
        from_sibling(0)

        def o_copy(i):
            return remote(o_send.at[layer, i], o_full.at[layer, me.kv_local], so.at[layer, i], ro.at[layer, me.kv_local], me.source(i), me.mem[2])

        lax.fori_loop(0, 4, lambda i, carry: attn_start(i, q_all[layer, i], state) or carry, 0)
        def early(n, carry):
            attn_early(n, kv, state)
            for e in FOUR:
                @pl.when(n == e)
                def _():
                    for which, number in EVENTS[N_TILES + e]:
                        step(which, number)
                    if e == 1:
                        from_sibling(1)
            return carry

        lax.fori_loop(0, 4, early, 0)

        def query(i, carry):
            @pl.when(i == 2)
            def _():
                from_sibling(2)

            o_send[layer, i] = attn_block(i, me.source(i), kv, state)

            @pl.when(i == 0)
            def _():
                for part, number in EVENTS[N_TILES + 4]:
                    step(part, number)

            @pl.when(me.s_self(i) == 0)
            def _():
                o_copy(i).start()

            @pl.when(me.s_self(i) == 1)
            def _():
                o_full[layer, me.kv_local] = o_send[layer, i]
            return carry

        lax.fori_loop(0, 4, query, 0)
        for n in range(BEFORE, N_TILES):
            tile(n)
        d_copy(layer, N_TILES - 1).wait()
        add_down(hid[:], N_TILES - 1)

        @pl.when(layer == 0)
        def _():
            first_tiles(1)

        o_cp.wait()
        for_others(me.t_self, lambda t: remote(o_send.at[layer, 0], o_full.at[layer, t], so.at[layer, 0], ro.at[layer, t], me.seq, sib).wait_recv())

        def p_copy(n):
            return remote(mlp.at[layer, n], part_in.at[layer, n], sp.at[layer], rp.at[layer, n], me.seq, sib)

        heads = jnp.concatenate([o_full[layer, t] for t in FOUR], axis=1)
        for n in range(0, 8, 2):
            d = jnp.dot(heads, wob[:, n * TOK:(n + 2) * TOK], preferred_element_type=F32)
            for e in range(2):
                mlp[layer, n + e] += d[:, e * TOK:(e + 1) * TOK]
                p_copy(n + e).start()
        for n in range(8):
            cols = pl.ds(n * TOK, TOK)
            p_copy(n).wait_recv()
            y = (mlp[layer, n] + part_in[layer, n]).astype(BF16)
            x_ref[:, cols] = (x_ref[:, cols].astype(F32) + y.astype(F32)).astype(BF16)
        return carry

    lax.fori_loop(0, 2, layer_body, 0)

    def drain(layer, carry):
        def gone(src, sem):
            remote(src, src, sem, rp.at[layer, 0], me.seq, sib).wait_send()

        for_others(me.t_self, lambda t: gone(kv_send.at[layer, t], skv.at[layer, t]))
        for_others(me.t_self, lambda t: gone(q_send.at[layer, t], sq.at[layer, t]))
        for_others(me.s_self, lambda i: gone(o_send.at[layer, i], so.at[layer, i]))
        gone(kv_all.at[layer, pl.ds(0, 26)], sag.at[layer])

        @pl.when(me.mem[2] == 0)
        def _():
            for t in FOUR:
                gone(kv_send.at[layer, t], skv.at[layer, 4 + t])
        gone(kv_all.at[layer, pl.ds(0, 32)], sdd.at[layer])
        gone(mlp.at[layer], sp.at[layer])
        return carry

    lax.fori_loop(0, 2, drain, 0)


def finish_kernel(x_in, k_in, v_in, x_out, k_out, v_out, sem):
    cps = [pltpu.make_async_copy(a, b, sem.at[n]) for n, (a, b) in enumerate(((x_in, x_out), (k_in, k_out), (v_in, v_out)))]
    for c in cps:
        c.start()
    for c in cps:
        c.wait()


def vmem(*shape, dtype=BF16):
    return pltpu.VMEM(shape, dtype)


BEFORE = 15
EVENTS = {5: ((0, 0),), 7: ((1, 0),), 9: ((0, 2),), 11: ((1, 2),), 12: ((2, 0),), 13: ((0, 4),), 15: (), 16: ((1, 4), (2, 1)), 17: (), 18: ((2, 2),), 19: (), 20: ((2, 4),)}


SCRATCH = [
    vmem(32, TOK, dtype=F32), vmem(32, TOK, dtype=F32), vmem(TOK, DM), vmem(2, 4, TOK, TOK), vmem(2, 4, TOK, LN), vmem(2, 4, TOK, TOK), vmem(2, HD, TOK, LN),
    vmem(2, 4, TOK, TOK), vmem(2, 4, TOK, TOK), vmem(2, 8, TOK, TOK, dtype=F32), vmem(2, 8, TOK, TOK, dtype=F32), vmem(TOK, TOK),
    vmem(QW, DM), vmem(2 * TOK, DM), vmem(3, DM, TOK), vmem(3, DM, TOK), vmem(3, TOK, DM), vmem(QW, DM),
    vmem(4, LN, QW), vmem(4, LN, QW), vmem(4, 8, QW, dtype=F32), vmem(4, RC, QW, dtype=F32), vmem(4, HD, QW, dtype=F32), vmem(2 * TK, QW, dtype=F32), vmem(2 * RC, QW, dtype=F32),
] + [pltpu.SemaphoreType.DMA(s) for s in ((1,), (3,), (3, 3), (1,), (2, 8), (2, 4), (2,), (2,), (2, 4), (2,), (2, 4), (2, 4), (2, 4, 7), (2, 3), (2, 4), (2, 8))]


def solution(mesh):
    row_spec = P(('batch', 'seq'), None)
    pos_spec = P(('batch', 'seq'))
    head_spec = P(None, None, 'head', None)
    out_proj_spec = P(None, 'head', None, None)
    col_spec = P(None, None, 'head')
    down_spec = P(None, 'head', None)
    cache_spec = P(None, ('batch', 'seq'), 'head', None)
    in_vmem = pl.BlockSpec(memory_space=pltpu.VMEM)
    anywhere = pl.BlockSpec(memory_space=pl.ANY)

    def local_forward(x, pos, w_q, w_k, w_v, w_o, w_gate, w_up, w_down, gain):
        wq = w_q.transpose(0, 2, 3, 1).reshape(2, QW, DM)
        wk = w_k.transpose(0, 2, 3, 1).reshape(2, TOK, DM)
        wv = w_v.transpose(0, 2, 3, 1).reshape(2, TOK, DM)
        wo = w_o.reshape(2, QW, DM)
        x, kT, vT = pl.pallas_call(
            stack_kernel,
            out_shape=tuple(pltpu.VMEM(s, BF16) for s in OUT_SHAPES),
            in_specs=[anywhere] + [in_vmem] * 2 + [anywhere] * 7,
            out_specs=(in_vmem,) * 3,
            scratch_shapes=SCRATCH,
            compiler_params=pltpu.CompilerParams(collective_id=0, has_side_effects=True, vmem_limit_bytes=VMEM_LIMIT),
            name='stack',
        )(x, gain, pos.reshape(1, TOK), wq, wk, wv, w_gate, w_up, w_down, wo)
        x, kT, vT = pl.pallas_call(
            finish_kernel,
            out_shape=tuple(jax.ShapeDtypeStruct(s, BF16) for s in OUT_SHAPES),
            in_specs=[in_vmem] * 3,
            out_specs=(anywhere,) * 3,
            scratch_shapes=[pltpu.SemaphoreType.DMA((3,))],
            compiler_params=pltpu.CompilerParams(vmem_limit_bytes=QW * QW),
            name='finish',
        )(*[pltpu.with_memory_space_constraint(a, pltpu.VMEM) for a in (x, kT, vT)])
        k_cache = kT.reshape(2, 4, HD, TOK).transpose(0, 3, 1, 2)
        v_cache = vT.reshape(2, 4, HD, TOK).transpose(0, 3, 1, 2)
        return x, k_cache, v_cache

    return jax.shard_map(local_forward, mesh=mesh, in_specs=(row_spec, pos_spec, head_spec, head_spec, head_spec, out_proj_spec, col_spec, col_spec, down_spec, P(None, None)), out_specs=(row_spec, cache_spec, cache_spec), check_vma=False)


OUT_SHAPES = ((TOK, DM), (2, TOK, TOK), (2, TOK, TOK))
```

```python
import functools
import jax
import jax.numpy as jnp
from jax import lax
from jax.experimental import pallas as pl
from jax.experimental.pallas import tpu as pltpu
from jax.sharding import PartitionSpec as P

ROPE_BASE = 500000.0
EPS = 1e-5
LOG2E = 1.4426950408889634
NEG = -1e30
MESH = pl.DeviceIdType.MESH
TOK, DM, QW, LN, HD = 256, 2048, 1024, 128, 64
F32 = jnp.float32
BF16 = jnp.bfloat16
VMEM_LIMIT = 62 * 1024 * 1024

STRIDE = (1, 4, 16)
N_TILES = 16
NB = 4
TK = NB * TOK
HALF = NB * LN
RC = 8
NT = (((1,), (1,)), ((), ()))
PARTS = ((0,), (1,), (2, 3))
SENDS = ((0, ()), (1, ()), (1, (0,)), (2, ()), (2, (0,)), (2, (1,)), (2, (0, 1)))
SECOND, THIRD = (1, 2), (3, 4, 5, 6)
NEXT = ((2, 4), (5,), (6,), (), (), (), ())
FOUR, TWO, EIGHT = range(4), range(2), range(8)


class Place:
    def __init__(self):
        self.seq = lax.axis_index('seq')
        self.head = lax.axis_index('head')
        self.xyz = (self.seq % 4, (self.seq // 4) % 4, self.seq // 16)
        self.mem = tuple(c // 2 for c in self.xyz)
        self.cls = tuple(((c + 1) // 2) % 2 for c in self.xyz)
        self.core = (self.mem[0] + self.mem[1]) % 2
        self.kv_local = 2 * self.mem[1] + self.mem[0]
        self.member = 2 * self.mem[2] + self.mem[1]
        same_z = 1 - lax.rem(self.head + self.mem[2], 2)
        self.own = 1 - lax.rem(self.head + self.core, 2)
        self.flag = same_z * self.own

    def at(self, mem):
        cs = [m * 3 + c * (1 - 2 * m) for m, c in zip(mem, self.cls)]
        return cs[2] * 16 + cs[1] * 4 + cs[0]

    def target(self, t):
        return self.at((t % 2, t // 2, self.head))

    def source_mem(self, i):
        my = i % 2
        return ((my + self.head) % 2, my, i // 2)

    def source(self, i):
        return self.at(self.source_mem(i))

    def steps(self, i, mem):
        d = [(1 - 2 * c) * (1 - 2 * m) * s for c, m, s in zip(self.cls, mem, STRIDE)]
        turns = [d[k:] + d[:k] for k in range(3)]
        first, other = ((0, 1), (2, 0), (1, 1), (2, 2))[i]
        return [a * (1 - self.head) + b * self.head for a, b in zip(turns[first], turns[other])]

    def across(self, i, crossed):
        steps = self.steps(i, self.source_mem(i))
        return functools.reduce(lambda a, d: a + steps[d], crossed, self.source(i))

    def second(self, t):
        mem = (t % 2, t // 2, self.head)
        d = [(1 - 2 * c) * (1 - 2 * m) * s for c, m, s in zip(self.cls, mem, STRIDE)]
        low = d[0] * (1 - self.core) + d[1] * self.core
        high = d[2] * (1 - self.core) + d[0] * self.core
        return self.at(mem) + low * (1 - self.mem[1]) + high * self.mem[1]

    def is_member(self, i):
        return (1 - lax.rem(i // 2 + self.mem[2], 2)) * (1 - lax.rem(i % 2 + self.mem[1], 2))

    def s_self(self, i):
        return self.flag * self.is_member(i)

    def o_self(self, h):
        return self.own * self.is_member(h // 2) * (1 - lax.rem(h % 2 + self.mem[0], 2))

    def t_self(self, t):
        return self.flag * (1 - lax.rem(t // 2 + self.mem[1], 2)) * (1 - lax.rem(t % 2 + self.mem[0], 2))


def fold_max(x):
    return jnp.max(x.reshape(x.shape[0] // RC, RC, x.shape[1]), axis=0)


def fold_sum(x):
    return jnp.sum(x.reshape(x.shape[0] // RC, RC, x.shape[1]), axis=0)


def attn_logits(first, c, kv_all, qa, qb, sbuf, off, mx_ref, moff):
    cols = pl.ds(c * TOK, TOK)
    keys = kv_all[pl.ds(first, NB), :LN, :].reshape(HALF, LN)
    sa = jnp.dot(keys, qa[:, cols], preferred_element_type=F32) * (LOG2E / 8.0)
    sb = jnp.dot(keys, qb[:, cols], preferred_element_type=F32) * (LOG2E / 8.0)
    sbuf[pl.ds(off, HALF), cols] = sa
    sbuf[pl.ds(off + HALF, HALF), cols] = sb
    mx_ref[pl.ds(moff, RC), cols] = jnp.maximum(fold_max(sa), fold_max(sb))


def attn_update(cols, mx, parts, vTs, m_ref, l_ref, acc_ref):
    m_old = m_ref[0:1, cols]
    m_new = jnp.maximum(m_old, jnp.max(mx, axis=0, keepdims=True))
    alpha = jnp.exp2(m_old - m_new)
    m_ref[:, cols] = jnp.broadcast_to(m_new, (8, TOK))
    lsum = l_ref[:, cols] * alpha
    ps = []
    for s in parts:
        p = jnp.exp2(s - m_new)
        lsum = lsum + fold_sum(p)
        ps.append(p.astype(BF16))
    l_ref[:, cols] = lsum
    pv = jnp.dot(jnp.concatenate(vTs, axis=1), jnp.concatenate(ps, axis=0), preferred_element_type=F32)
    acc_ref[:, cols] = acc_ref[:, cols] * alpha + pv


def values_of(kv_all, first, blocks):
    return [kv_all[first + b, LN + HD * h:192 + HD * h, :] for h in TWO for b in range(blocks)]


def attn_tail(first, t, kv_all, sbuf, off, m_ref, l_ref, acc_ref):
    for c in FOUR:
        cols = pl.ds(c * TOK, TOK)
        ti = lax.broadcasted_iota(jnp.int32, (LN, TOK), 1)
        ki = lax.broadcasted_iota(jnp.int32, (LN, TOK), 0)
        parts = []
        for h in TWO:
            base = pl.multiple_of(off + h * HALF, LN)
            if t > 0:
                parts.append(sbuf[pl.ds(base, t * LN), cols])
            parts.append(jnp.where(ki + h * LN <= ti, sbuf[pl.ds(base + t * LN, LN), cols], NEG))
        mx = functools.reduce(jnp.maximum, [fold_max(p) for p in parts])
        attn_update(cols, mx, parts, values_of(kv_all, first, t + 1), m_ref, l_ref, acc_ref)


def attn_start(i, qT, state):
    qa, qb, m_ref, l_ref, acc_ref, _, _ = state
    zero = jnp.zeros((HD, TOK), BF16)
    for g in FOUR:
        q = qT[g * HD:(g + 1) * HD, :]
        cols = pl.ds(g * TOK, TOK)
        qa[i, :, cols] = jnp.concatenate([q, zero], axis=0)
        qb[i, :, cols] = jnp.concatenate([zero, q], axis=0)
    m_ref[i] = jnp.full((8, QW), NEG, F32)
    l_ref[i] = jnp.zeros((RC, QW), F32)
    acc_ref[i] = jnp.zeros((HD, QW), F32)


def attn_step(now, then, p, kv, state):
    qa, qb, m_ref, l_ref, acc_ref, sbuf, mx_ref = state
    i, group = now
    j, after = then
    for c in FOUR:
        attn_logits(after * NB, c, kv, qa.at[j], qb.at[j], sbuf, (1 - p) * TK, mx_ref, (1 - p) * RC)
        cols = pl.ds(c * TOK, TOK)
        attn_update(cols, mx_ref[pl.ds(p * RC, RC), cols], [sbuf[pl.ds(p * TK, TK), cols]], values_of(kv, group * NB, NB), m_ref.at[i], l_ref.at[i], acc_ref.at[i])


def attn_prime(i, group, kv, state):
    qa, qb, _, _, _, sbuf, mx_ref = state
    for c in FOUR:
        attn_logits(group * NB, c, kv, qa.at[i], qb.at[i], sbuf, 0, mx_ref, 0)


def attn_early(n, kv, state):
    def at(s):
        s = 4 * n + s
        more = 1 - s // 16
        return (2 + s // 4 % 2) * more, ((s % 4) // 2 * 4 + 2 * (s // 8) + s % 2) * more

    @pl.when(n % 2 == 0)
    def _():
        attn_prime(2, n, kv, state)
    for e in FOUR:
        ahead = at(e + 1) if e < 3 else tuple(jnp.where(n == 1, a, b) for a, b in zip(at(e), at(e + 1)))
        attn_step(at(e), ahead, e % 2, kv, state)


def attn_block(i, pos, kv, state):
    qa, qb, m_ref, l_ref, acc_ref, sbuf, mx_ref = state
    first = i // 2 * 8
    groups = pos // NB - first

    @pl.when(i > 0)
    def _():
        attn_prime(i, first, kv, state)

    def one(n, p):
        attn_step((i, first + n), (i, first + n + 1), p, kv, state)

    done = groups // 4 * 4

    @pl.when(groups >= 4)
    def _():
        for n in FOUR:
            one(n, n % 2)

    @pl.when(groups - done >= 2)
    def _():
        one(done, 0)
        one(done + 1, 1)

    @pl.when(groups % 2 == 1)
    def _():
        one(groups - 1, 0)
    for t in range(NB):
        @pl.when(pos % NB == t)
        def _():
            attn_tail(pos // NB * NB, t, kv, sbuf, (groups % 2) * TK, m_ref.at[i], l_ref.at[i], acc_ref.at[i])
    oT = acc_ref[i] * (1.0 / jnp.sum(l_ref[i], axis=0, keepdims=True))
    halves = []
    for g in range(0, 4, 2):
        two = jnp.concatenate([oT[:, g * TOK:(g + 1) * TOK], oT[:, (g + 1) * TOK:(g + 2) * TOK]], axis=0)
        halves.append(two.T.astype(BF16))
    return jnp.concatenate(halves, axis=1)


def stack_kernel(x_hbm, gain_ref, pos_ref, wq, wk, wv, wg, wu, wd, wo, x_ref, k_ref, v_ref,
                 cosT, sinT, h_ref, q_send, kv_send, q_all, kv_all, o_send, o_full, mlp, part_in, hid, wqb, wkvb, wgb, wub, wdb, wob,
                 qa, qb, m_ref, l_ref, acc_ref, sbuf, mx_ref,
                 xsem, wsem, msem, osem, skv, sq, sag, sdd, so, sp, rkv, rq, rag, rdd, ro, rp):
    me = Place()
    sib = 1 - me.head
    state = (qa, qb, m_ref, l_ref, acc_ref, sbuf, mx_ref)

    def remote(src, dst, ssem, rsem, seq, head):
        return pltpu.make_async_remote_copy(src_ref=src, dst_ref=dst, send_sem=ssem, recv_sem=rsem, device_id={'seq': seq, 'head': head}, device_id_type=MESH)

    def for_others(is_self, fn):
        for i in FOUR:
            @pl.when(is_self(i) == 0)
            def _():
                fn(i)

    start_cps = [pltpu.make_async_copy(x_hbm, x_ref, xsem.at[0])]

    def proj_copies(layer):
        return (pltpu.make_async_copy(wk.at[layer], wkvb.at[pl.ds(0, TOK)], wsem.at[0]), pltpu.make_async_copy(wv.at[layer], wkvb.at[pl.ds(TOK, TOK)], wsem.at[1]), pltpu.make_async_copy(wq.at[layer], wqb, wsem.at[2]))

    for c in start_cps:
        c.start()
    for n in TWO:
        proj_copies(0)[n].start()

    barrier = pltpu.get_barrier_semaphore()

    def hello(seq, head):
        pl.semaphore_signal(barrier, inc=1, device_id={'seq': seq, 'head': head}, device_id_type=MESH)

    for_others(me.s_self, lambda i: hello(me.source(i), me.mem[2]))
    for h in EIGHT:
        @pl.when(me.o_self(h) == 0)
        def _():
            hello(me.at((h % 2, h // 2 % 2, h // 4)), me.core)
    for i in TWO:
        hello(me.across(i, (0,)), me.mem[2])
    for step in me.steps(0, me.mem):
        hello(me.seq + step, me.head)
    hello(me.seq, sib)

    def gu_copies(layer, n):
        off = pl.multiple_of(n * TOK, TOK)
        slot = n % 3
        return (pltpu.make_async_copy(wg.at[layer, :, pl.ds(off, TOK)], wgb.at[slot], msem.at[0, slot]), pltpu.make_async_copy(wu.at[layer, :, pl.ds(off, TOK)], wub.at[slot], msem.at[1, slot]))

    def d_copy(layer, n):
        return pltpu.make_async_copy(wd.at[layer, pl.ds(pl.multiple_of(n * TOK, TOK), TOK)], wdb.at[n % 3], msem.at[2, n % 3])

    def first_tiles(layer):
        for n in range(3):
            for c in gu_copies(layer, n):
                c.start()
        for n in TWO:
            d_copy(layer, n).start()

    freq = ROPE_BASE ** (-(lax.broadcasted_iota(jnp.int32, (HD // 2, TOK), 0).astype(F32) * 2.0 / HD))
    angles = pos_ref[:].astype(F32) * freq
    cosT[:] = jnp.cos(angles)
    sinT[:] = jnp.sin(angles)
    for c in start_cps:
        c.wait()
    proj_copies(0)[2].start()

    def rope(a):
        lo, hi = a[:32], a[32:HD]
        return jnp.concatenate([lo * cosT[:] - hi * sinT[:], hi * cosT[:] + lo * sinT[:]], axis=0)

    def project(w):
        return lax.dot_general(w, h_ref[:], NT, preferred_element_type=F32).astype(BF16)

    def layer_body(layer, carry):
        kv = kv_all.at[layer]
        xf = x_ref[:].astype(F32)
        inv = lax.rsqrt(jnp.mean(xf * xf, axis=-1, keepdims=True) + EPS)
        gain = jnp.where(layer == 0, gain_ref[0:1, :].astype(F32), gain_ref[1:2, :].astype(F32))
        h_ref[:] = (xf * inv * gain).astype(BF16)

        w_cps = proj_copies(layer)
        w_cps[0].wait()
        w_cps[1].wait()
        kT = project(wkvb[:TOK])
        vT = project(wkvb[TOK:])
        for t in FOUR:
            k = rope(kT[t * HD:(t + 1) * HD].astype(F32)).astype(BF16)
            k_ref[layer, t * HD:(t + 1) * HD, :] = k
            kf = k.astype(F32)
            kv_send[layer, t, :LN, :] = jnp.concatenate([kf[:, :LN], kf[:, LN:TOK]], axis=0).T.astype(BF16)
            v = vT[t * HD:(t + 1) * HD]
            v_ref[layer, t * HD:(t + 1) * HD, :] = v
            kv_send[layer, t, LN:LN + HD, :] = v[:, :LN]
            kv_send[layer, t, LN + HD:TOK, :] = v[:, LN:TOK]

        @pl.when(layer == 0)
        def _():
            first_tiles(0)

        @pl.when(layer == 0)
        def _():
            pl.semaphore_wait(barrier, 16 - me.flag - me.own + 4 * (1 - me.mem[2]))

        def kv_copy(t):
            return remote(kv_send.at[layer, t], kv.at[me.seq], skv.at[layer, t], rkv.at[layer, me.member], me.target(t), me.core)

        def q_copy(t):
            return remote(q_send.at[layer, t], q_all.at[layer, me.member], sq.at[layer, t], rq.at[layer, me.member], me.target(t), me.core)

        def second_copy(t):
            return remote(kv_send.at[layer, t], kv.at[me.seq], skv.at[layer, 4 + t], rag.at[layer, me.mem[1], 0], me.second(t), me.core)

        for_others(me.t_self, lambda t: kv_copy(t).start())

        @pl.when(me.mem[2] == 0)
        def _():
            for t in FOUR:
                second_copy(t).start()
        for t in FOUR:
            @pl.when(me.t_self(t) == 1)
            def _():
                kv[me.seq] = kv_send[layer, t]

        w_cps[2].wait()
        for t in FOUR:
            qT = project(wqb[t * TOK:(t + 1) * TOK])
            for g in FOUR:
                q_send[layer, t, g * HD:(g + 1) * HD, :] = rope(qT[g * HD:(g + 1) * HD].astype(F32)).astype(BF16)

        def send_queries():
            for_others(me.t_self, lambda t: q_copy(t).start())
            for t in FOUR:
                @pl.when(me.t_self(t) == 1)
                def _():
                    q_all[layer, me.member] = q_send[layer, t]

        def ag(i, k):
            dim, crossed = SENDS[k]
            block = kv.at[me.across(i, crossed)]
            return remote(block, block, sag.at[layer], rag.at[layer, i, k], me.seq + me.steps(i, me.mem)[dim], me.head)

        def relay(i, crossed):
            block = kv.at[me.across(i, crossed)]
            remote(block, block, sdd.at[layer], rdd.at[layer, min(i, 2)], me.seq, sib).start()

        def arrived(i, k):
            dim, crossed = SENDS[k]
            block = kv.at[me.across(i, crossed + (dim,))]
            remote(block, block, sag.at[layer], rag.at[layer, i, k], me.seq, sib).wait_recv()

        def step(part, number):
            members = PARTS[part]
            if number == 0:
                for i in members:
                    @pl.when(me.s_self(i) == 0)
                    def _():
                        remote(kv_send.at[layer, 0], kv.at[me.source(i)], skv.at[layer, 0], rkv.at[layer, i], me.seq, sib).wait_recv()
                for k in ((1, 3) if part < 2 else (0, 1, 3)):
                    for i in members:
                        ag(i, k).start()
                for i in members:
                    relay(i, ())
            first = (0,) if number == (part == 2) else ()
            waits = first if number < 2 else SECOND if number == 2 else THIRD
            for k in waits:
                for i in members:
                    arrived(i, k)
                    for nxt in NEXT[k]:
                        ag(i, nxt).start()
            for k in waits:
                for i in members:
                    relay(i, SENDS[k][1] + (SENDS[k][0],))

        def from_sibling(part):
            blocks = kv.at[pl.ds(0, 8 * len(PARTS[part]))]
            remote(blocks, blocks, sdd.at[layer], rdd.at[layer, part], me.seq, sib).wait_recv()

        def gate_up(n):
            g = jnp.dot(h_ref[:], wgb[n % 3], preferred_element_type=F32)
            u = jnp.dot(h_ref[:], wub[n % 3], preferred_element_type=F32)
            return (g * jax.nn.sigmoid(g) * u).astype(BF16)

        def add_down(hidden, n):
            d = jnp.dot(hidden, wdb[n % 3], preferred_element_type=F32)
            for c in EIGHT:
                part = d[:, c * TOK:(c + 1) * TOK]
                mlp[layer, c] = part if n == 0 else mlp[layer, c] + part

        for c in gu_copies(layer, 0):
            c.wait()
        hid[:] = gate_up(0)
        for c in gu_copies(layer, 3):
            c.start()
        d_copy(layer, 2).start()

        def tile(n):
            for c in gu_copies(layer, n):
                c.wait()
            d_copy(layer, n - 1).wait()
            before = hid[:]
            now = gate_up(n)
            add_down(before, n - 1)
            hid[:] = now
            if n + 3 < N_TILES:
                for c in gu_copies(layer, n + 3):
                    c.start()
            if n + 2 < N_TILES:
                d_copy(layer, n + 2).start()

        for n in range(1, N_TILES):
            for part, number in EVENTS.get(n, ()):
                step(part, number)
            if n == 4:
                send_queries()
            tile(n)
        d_copy(layer, N_TILES - 1).wait()
        add_down(hid[:], N_TILES - 1)

        p_copy = remote(mlp.at[layer], part_in.at[layer], sp.at[layer], rp.at[layer], me.seq, sib)
        p_copy.start()
        half = pl.ds(pl.multiple_of(me.head * QW, QW), QW)
        o_cp = pltpu.make_async_copy(wo.at[layer], wob.at[half], osem.at[0])
        o_cp.start()
        wo_copy = remote(wob.at[half], wob.at[half], osem.at[1], osem.at[2], me.seq, sib)

        @pl.when(layer == 0)
        def _():
            for c in proj_copies(1):
                c.start()
            first_tiles(1)
        for_others(me.s_self, lambda i: remote(q_send.at[layer, 0], q_all.at[layer, i], sq.at[layer, 0], rq.at[layer, i], me.seq, sib).wait_recv())
        from_sibling(0)

        def o_copy(i, head):
            h = 4 * me.mem[2] + me.kv_local
            return remote(o_send.at[layer, i], o_full.at[layer, h], so.at[layer, i, head], ro.at[layer, h], me.source(i), head)

        def for_outputs(i, fn, at_home):
            own = me.own * me.is_member(i)
            for head in TWO:
                here = own * (1 - lax.rem(me.head + head, 2))

                @pl.when(here == 0)
                def _():
                    fn(i, head)

                @pl.when(here == 1)
                def _():
                    at_home(i)

        lax.fori_loop(0, 4, lambda i, carry: attn_start(i, q_all[layer, i], state) or carry, 0)
        def early(n, carry):
            attn_early(n, kv, state)
            for e in FOUR:
                @pl.when(n == e)
                def _():
                    for which, number in BREAKS[e]:
                        step(which, number)
                    if e == 0:
                        o_cp.wait()
                        wo_copy.start()
                    if e == 1:
                        from_sibling(1)
            return carry

        lax.fori_loop(0, 4, early, 0)

        def query(i, carry):
            @pl.when(i == 2)
            def _():
                from_sibling(2)

            o_send[layer, i] = attn_block(i, me.source(i), kv, state)

            @pl.when(i == 0)
            def _():
                for part, number in BREAKS[4]:
                    step(part, number)

            def keep(i):
                o_full[layer, 4 * me.mem[2] + me.kv_local] = o_send[layer, i]

            for_outputs(i, lambda i, head: o_copy(i, head).start(), keep)
            return carry

        lax.fori_loop(0, 4, query, 0)

        wo_copy.wait_send()
        other = pl.ds(pl.multiple_of(sib * QW, QW), QW)
        remote(wob.at[other], wob.at[other], osem.at[1], osem.at[2], me.seq, sib).wait_recv()
        p_copy.wait_recv()
        for h in EIGHT:
            @pl.when(me.o_self(h) == 0)
            def _():
                remote(o_send.at[layer, 0], o_full.at[layer, h], so.at[layer, 0, 0], ro.at[layer, h], me.seq, sib).wait_recv()

        heads = jnp.concatenate([o_full[layer, h] for h in EIGHT], axis=1)
        for n in range(0, 8, 2):
            d = jnp.dot(heads, wob[:, n * TOK:(n + 2) * TOK], preferred_element_type=F32)
            for e in TWO:
                cols = pl.ds((n + e) * TOK, TOK)
                y = (mlp[layer, n + e] + part_in[layer, n + e] + d[:, e * TOK:(e + 1) * TOK]).astype(BF16)
                x_ref[:, cols] = (x_ref[:, cols].astype(F32) + y.astype(F32)).astype(BF16)
        return carry

    lax.fori_loop(0, 2, layer_body, 0)

    def drain(layer, carry):
        def gone(src, sem):
            remote(src, src, sem, rp.at[layer], me.seq, sib).wait_send()

        for_others(me.t_self, lambda t: gone(kv_send.at[layer, t], skv.at[layer, t]))
        for_others(me.t_self, lambda t: gone(q_send.at[layer, t], sq.at[layer, t]))
        for i in FOUR:
            for head in TWO:
                here = me.own * me.is_member(i) * (1 - lax.rem(me.head + head, 2))

                @pl.when(here == 0)
                def _():
                    gone(o_send.at[layer, i], so.at[layer, i, head])
        gone(kv_all.at[layer, pl.ds(0, 26)], sag.at[layer])

        @pl.when(me.mem[2] == 0)
        def _():
            for t in FOUR:
                gone(kv_send.at[layer, t], skv.at[layer, 4 + t])
        gone(kv_all.at[layer, pl.ds(0, 32)], sdd.at[layer])
        gone(mlp.at[layer], sp.at[layer])
        return carry

    lax.fori_loop(0, 2, drain, 0)


def finish_kernel(x_in, k_in, v_in, x_out, k_out, v_out, sem):
    cps = [pltpu.make_async_copy(a, b, sem.at[n]) for n, (a, b) in enumerate(((x_in, x_out), (k_in, k_out), (v_in, v_out)))]
    for c in cps:
        c.start()
    for c in cps:
        c.wait()


def vmem(*shape, dtype=BF16):
    return pltpu.VMEM(shape, dtype)


EVENTS = {5: ((0, 0),), 9: ((0, 2), (1, 0)), 12: ((1, 2), (2, 0)), 13: ((0, 4),)}
BREAKS = (((1, 4), (2, 1)), (), ((2, 2),), (), ((2, 4),))


SCRATCH = [
    vmem(32, TOK, dtype=F32), vmem(32, TOK, dtype=F32), vmem(TOK, DM), vmem(2, 4, TOK, TOK), vmem(2, 4, TOK, LN), vmem(2, 4, TOK, TOK), vmem(2, HD, TOK, LN),
    vmem(2, 4, TOK, TOK), vmem(2, 8, TOK, TOK), vmem(2, 8, TOK, TOK, dtype=F32), vmem(2, 8, TOK, TOK, dtype=F32), vmem(TOK, TOK),
    vmem(QW, DM), vmem(2 * TOK, DM), vmem(3, DM, TOK), vmem(3, DM, TOK), vmem(3, TOK, DM), vmem(DM, DM),
    vmem(4, LN, QW), vmem(4, LN, QW), vmem(4, 8, QW, dtype=F32), vmem(4, RC, QW, dtype=F32), vmem(4, HD, QW, dtype=F32), vmem(2 * TK, QW, dtype=F32), vmem(2 * RC, QW, dtype=F32),
] + [pltpu.SemaphoreType.DMA(s) for s in ((1,), (3,), (3, 3), (3,), (2, 8), (2, 4), (2,), (2,), (2, 4, 2), (2,), (2, 4), (2, 4), (2, 4, 7), (2, 3), (2, 8), (2,))]


def solution(mesh):
    row_spec = P(('batch', 'seq'), None)
    pos_spec = P(('batch', 'seq'))
    head_spec = P(None, None, 'head', None)
    out_proj_spec = P(None, 'head', None, None)
    col_spec = P(None, None, 'head')
    down_spec = P(None, 'head', None)
    cache_spec = P(None, ('batch', 'seq'), 'head', None)
    in_vmem = pl.BlockSpec(memory_space=pltpu.VMEM)
    anywhere = pl.BlockSpec(memory_space=pl.ANY)

    def local_forward(x, pos, w_q, w_k, w_v, w_o, w_gate, w_up, w_down, gain):
        wq = w_q.transpose(0, 2, 3, 1).reshape(2, QW, DM)
        wk = w_k.transpose(0, 2, 3, 1).reshape(2, TOK, DM)
        wv = w_v.transpose(0, 2, 3, 1).reshape(2, TOK, DM)
        wo = w_o.reshape(2, QW, DM)
        x, kT, vT = pl.pallas_call(
            stack_kernel,
            out_shape=tuple(pltpu.VMEM(s, BF16) for s in OUT_SHAPES),
            in_specs=[anywhere] + [in_vmem] * 2 + [anywhere] * 7,
            out_specs=(in_vmem,) * 3,
            scratch_shapes=SCRATCH,
            compiler_params=pltpu.CompilerParams(collective_id=0, has_side_effects=True, vmem_limit_bytes=VMEM_LIMIT),
            name='stack',
        )(x, gain, pos.reshape(1, TOK), wq, wk, wv, w_gate, w_up, w_down, wo)
        x, kT, vT = pl.pallas_call(
            finish_kernel,
            out_shape=tuple(jax.ShapeDtypeStruct(s, BF16) for s in OUT_SHAPES),
            in_specs=[in_vmem] * 3,
            out_specs=(anywhere,) * 3,
            scratch_shapes=[pltpu.SemaphoreType.DMA((3,))],
            compiler_params=pltpu.CompilerParams(vmem_limit_bytes=QW * QW),
            name='finish',
        )(*[pltpu.with_memory_space_constraint(a, pltpu.VMEM) for a in (x, kT, vT)])
        k_cache = kT.reshape(2, 4, HD, TOK).transpose(0, 3, 1, 2)
        v_cache = vT.reshape(2, 4, HD, TOK).transpose(0, 3, 1, 2)
        return x, k_cache, v_cache

    return jax.shard_map(local_forward, mesh=mesh, in_specs=(row_spec, pos_spec, head_spec, head_spec, head_spec, out_proj_spec, col_spec, col_spec, down_spec, P(None, None)), out_specs=(row_spec, cache_spec, cache_spec), check_vma=False)


OUT_SHAPES = ((TOK, DM), (2, TOK, TOK), (2, TOK, TOK))
```

```python
import functools
import jax
import jax.numpy as jnp
from jax import lax
from jax.experimental import pallas as pl
from jax.experimental.pallas import tpu as pltpu
from jax.sharding import PartitionSpec as P

ROPE_BASE = 500000.0
EPS = 1e-5
LOG2E = 1.4426950408889634
NEG = -3e38
MESH = pl.DeviceIdType.MESH
TOK, DM, QW, LN, HD = 256, 2048, 1024, 128, 64
F32 = jnp.float32
BF16 = jnp.bfloat16
VMEM_LIMIT = 62 * 1024 * 1024

STRIDE = (1, 4, 16)
N_TILES = 16
NB = 4
TK = NB * TOK
HALF = NB * LN
RC = 8
NT = (((1,), (1,)), ((), ()))
PARTS = ((0,), (1,), (2, 3))
SENDS = ((0, ()), (1, ()), (1, (0,)), (2, ()), (2, (0,)), (2, (1,)), (2, (0, 1)))
SECOND, THIRD = (1, 2), (3, 4, 5, 6)
NEXT = ((2, 4), (5,), (6,), (), (), (), ())
FOUR = range(4)


class Place:
    def __init__(self):
        self.seq = lax.axis_index('seq')
        self.head = lax.axis_index('head')
        self.xyz = (self.seq % 4, (self.seq // 4) % 4, self.seq // 16)
        self.mem = tuple(c // 2 for c in self.xyz)
        self.cls = tuple(((c + 1) // 2) % 2 for c in self.xyz)
        self.core = (self.mem[0] + self.mem[1]) % 2
        self.kv_local = 2 * self.mem[1] + self.mem[0]
        self.member = 2 * self.mem[2] + self.mem[1]
        same_z = 1 - lax.rem(self.head + self.mem[2], 2)
        self.flag = same_z * (1 - lax.rem(self.head + self.core, 2))

    def at(self, mem):
        cs = [m * 3 + c * (1 - 2 * m) for m, c in zip(mem, self.cls)]
        return cs[2] * 16 + cs[1] * 4 + cs[0]

    def target(self, t):
        return self.at((t % 2, t // 2, self.head))

    def source_mem(self, i):
        my = i % 2
        return ((my + self.head) % 2, my, i // 2)

    def source(self, i):
        return self.at(self.source_mem(i))

    def steps(self, i, mem):
        d = [(1 - 2 * c) * (1 - 2 * m) * s for c, m, s in zip(self.cls, mem, STRIDE)]
        turns = [d[k:] + d[:k] for k in range(3)]
        first, other = ((0, 1), (2, 0), (1, 1), (2, 2))[i]
        return [a * (1 - self.head) + b * self.head for a, b in zip(turns[first], turns[other])]

    def across(self, i, crossed):
        steps = self.steps(i, self.source_mem(i))
        return functools.reduce(lambda a, d: a + steps[d], crossed, self.source(i))

    def second(self, t):
        mem = (t % 2, t // 2, self.head)
        d = [(1 - 2 * c) * (1 - 2 * m) * s for c, m, s in zip(self.cls, mem, STRIDE)]
        low = d[0] * (1 - self.core) + d[1] * self.core
        high = d[2] * (1 - self.core) + d[0] * self.core
        return self.at(mem) + low * (1 - self.mem[1]) + high * self.mem[1]

    def s_self(self, i):
        return self.flag * (1 - lax.rem(i // 2 + self.mem[2], 2)) * (1 - lax.rem(i % 2 + self.mem[1], 2))

    def t_self(self, t):
        return self.flag * (1 - lax.rem(t // 2 + self.mem[1], 2)) * (1 - lax.rem(t % 2 + self.mem[0], 2))


def fold_max(x):
    return jnp.max(x.reshape(x.shape[0] // RC, RC, x.shape[1]), axis=0)


def fold_sum(x):
    return jnp.sum(x.reshape(x.shape[0] // RC, RC, x.shape[1]), axis=0)


def attn_logits(first, c, kv_all, qa, qb, sbuf, off, mx_ref, moff):
    cols = pl.ds(c * TOK, TOK)
    keys = kv_all[pl.ds(first, NB), 0:LN, :].reshape(HALF, LN)
    sa = jnp.dot(keys, qa[:, cols], preferred_element_type=F32) * (LOG2E / 8.0)
    sb = jnp.dot(keys, qb[:, cols], preferred_element_type=F32) * (LOG2E / 8.0)
    sbuf[pl.ds(off, HALF), cols] = sa
    sbuf[pl.ds(off + HALF, HALF), cols] = sb
    mx_ref[pl.ds(moff, RC), cols] = jnp.maximum(fold_max(sa), fold_max(sb))


def attn_update(cols, mx, parts, vTs, m_ref, l_ref, acc_ref):
    m_old = m_ref[0:1, cols]
    m_new = jnp.maximum(m_old, jnp.max(mx, axis=0, keepdims=True))
    alpha = jnp.exp2(m_old - m_new)
    m_ref[:, cols] = jnp.broadcast_to(m_new, (8, TOK))
    lsum = l_ref[:, cols] * alpha
    ps = []
    for s in parts:
        p = jnp.exp2(s - m_new)
        lsum = lsum + fold_sum(p)
        ps.append(p.astype(BF16))
    l_ref[:, cols] = lsum
    pv = jnp.dot(jnp.concatenate(vTs, axis=1), jnp.concatenate(ps, axis=0), preferred_element_type=F32)
    acc_ref[:, cols] = acc_ref[:, cols] * alpha + pv


def values_of(kv_all, first, blocks):
    return [kv_all[first + b, LN + HD * h:192 + HD * h, :] for h in range(2) for b in range(blocks)]


def attn_tail(first, t, kv_all, sbuf, off, m_ref, l_ref, acc_ref):
    for c in FOUR:
        cols = pl.ds(c * TOK, TOK)
        ti = lax.broadcasted_iota(jnp.int32, (LN, TOK), 1)
        ki = lax.broadcasted_iota(jnp.int32, (LN, TOK), 0)
        parts = []
        for h in range(2):
            base = pl.multiple_of(off + h * HALF, LN)
            if t > 0:
                parts.append(sbuf[pl.ds(base, t * LN), cols])
            parts.append(jnp.where(ki + h * LN <= ti, sbuf[pl.ds(base + t * LN, LN), cols], NEG))
        mx = functools.reduce(jnp.maximum, [fold_max(p) for p in parts])
        attn_update(cols, mx, parts, values_of(kv_all, first, t + 1), m_ref, l_ref, acc_ref)


def attn_start(i, qT, state):
    qa, qb, m_ref, l_ref, acc_ref, _, _ = state
    zero = jnp.zeros((HD, TOK), BF16)
    for g in FOUR:
        q = qT[g * HD:(g + 1) * HD, :]
        cols = pl.ds(g * TOK, TOK)
        qa[i, :, cols] = jnp.concatenate([q, zero], axis=0)
        qb[i, :, cols] = jnp.concatenate([zero, q], axis=0)
    m_ref[i] = jnp.full((8, QW), NEG, F32)
    l_ref[i] = jnp.zeros((RC, QW), F32)
    acc_ref[i] = jnp.zeros((HD, QW), F32)


def attn_step(now, then, p, kv, state):
    qa, qb, m_ref, l_ref, acc_ref, sbuf, mx_ref = state
    i, group = now
    j, after = then
    for c in FOUR:
        attn_logits(after * NB, c, kv, qa.at[j], qb.at[j], sbuf, (1 - p) * TK, mx_ref, (1 - p) * RC)
        cols = pl.ds(c * TOK, TOK)
        attn_update(cols, mx_ref[pl.ds(p * RC, RC), cols], [sbuf[pl.ds(p * TK, TK), cols]], values_of(kv, group * NB, NB), m_ref.at[i], l_ref.at[i], acc_ref.at[i])


def attn_prime(i, group, kv, state):
    qa, qb, _, _, _, sbuf, mx_ref = state
    for c in FOUR:
        attn_logits(group * NB, c, kv, qa.at[i], qb.at[i], sbuf, 0, mx_ref, 0)


def attn_early(n, kv, state):
    def at(s):
        s = 4 * n + s
        more = 1 - s // 16
        return (2 + s // 4 % 2) * more, ((s % 4) // 2 * 4 + 2 * (s // 8) + s % 2) * more

    @pl.when(n % 2 == 0)
    def _():
        attn_prime(2, n, kv, state)
    for e in FOUR:
        ahead = at(e + 1) if e < 3 else tuple(jnp.where(n == 1, a, b) for a, b in zip(at(e), at(e + 1)))
        attn_step(at(e), ahead, e % 2, kv, state)


def attn_block(i, pos, kv, state):
    qa, qb, m_ref, l_ref, acc_ref, sbuf, mx_ref = state
    first = i // 2 * 8
    groups = pos // NB - first

    @pl.when(i > 0)
    def _():
        attn_prime(i, first, kv, state)

    def one(n, p):
        attn_step((i, first + n), (i, first + n + 1), p, kv, state)

    done = groups // 4 * 4

    @pl.when(groups >= 4)
    def _():
        for n in FOUR:
            one(n, n % 2)

    @pl.when(groups - done >= 2)
    def _():
        one(done, 0)
        one(done + 1, 1)

    @pl.when(groups % 2 == 1)
    def _():
        one(groups - 1, 0)
    for t in range(NB):
        @pl.when(pos % NB == t)
        def _():
            attn_tail(pos // NB * NB, t, kv, sbuf, (groups % 2) * TK, m_ref.at[i], l_ref.at[i], acc_ref.at[i])
    oT = acc_ref[i] / jnp.sum(l_ref[i], axis=0, keepdims=True)
    halves = []
    for g in range(0, 4, 2):
        two = jnp.concatenate([oT[:, g * TOK:(g + 1) * TOK], oT[:, (g + 1) * TOK:(g + 2) * TOK]], axis=0)
        halves.append(two.T.astype(BF16))
    return jnp.concatenate(halves, axis=1)


def stack_kernel(x_hbm, gain_ref, pos_ref, wq, wk, wv, wg, wu, wd, wo, x_ref, k_ref, v_ref,
                 cosT, sinT, h_ref, q_send, kv_send, q_all, kv_all, o_send, o_full, mlp, part_in, hid, wqb, wkvb, wgb, wub, wdb, wob,
                 qa, qb, m_ref, l_ref, acc_ref, sbuf, mx_ref,
                 xsem, wsem, msem, osem, skv, sq, sag, sdd, so, sp, rkv, rq, rag, rdd, ro, rp):
    me = Place()
    sib = 1 - me.head
    state = (qa, qb, m_ref, l_ref, acc_ref, sbuf, mx_ref)

    def remote(src, dst, ssem, rsem, seq, head):
        return pltpu.make_async_remote_copy(src_ref=src, dst_ref=dst, send_sem=ssem, recv_sem=rsem, device_id={'seq': seq, 'head': head}, device_id_type=MESH)

    def for_others(is_self, fn):
        for i in FOUR:
            @pl.when(is_self(i) == 0)
            def _():
                fn(i)

    start_cps = [pltpu.make_async_copy(x_hbm, x_ref, xsem.at[0])]

    def proj_copies(layer):
        return (pltpu.make_async_copy(wk.at[layer], wkvb.at[pl.ds(0, TOK)], wsem.at[0]), pltpu.make_async_copy(wv.at[layer], wkvb.at[pl.ds(TOK, TOK)], wsem.at[1]), pltpu.make_async_copy(wq.at[layer], wqb, wsem.at[2]))

    for c in start_cps:
        c.start()
    for n in range(2):
        proj_copies(0)[n].start()

    barrier = pltpu.get_barrier_semaphore()

    def hello(seq, head):
        pl.semaphore_signal(barrier, inc=1, device_id={'seq': seq, 'head': head}, device_id_type=MESH)

    for_others(me.s_self, lambda i: hello(me.source(i), me.mem[2]))
    for_others(me.t_self, lambda t: hello(me.target(t), me.core))
    for i in range(2):
        hello(me.across(i, (0,)), me.mem[2])
    for step in me.steps(0, me.mem):
        hello(me.seq + step, me.head)
    hello(me.seq, sib)

    def gu_copies(layer, n):
        off = pl.multiple_of(n * TOK, TOK)
        slot = n % 3
        return (pltpu.make_async_copy(wg.at[layer, :, pl.ds(off, TOK)], wgb.at[slot], msem.at[0, slot]), pltpu.make_async_copy(wu.at[layer, :, pl.ds(off, TOK)], wub.at[slot], msem.at[1, slot]))

    def d_copy(layer, n):
        return pltpu.make_async_copy(wd.at[layer, pl.ds(pl.multiple_of(n * TOK, TOK), TOK)], wdb.at[n % 3], msem.at[2, n % 3])

    def first_tiles(layer):
        for n in range(3):
            for c in gu_copies(layer, n):
                c.start()
        for n in range(2):
            d_copy(layer, n).start()

    freq = ROPE_BASE ** (-(lax.broadcasted_iota(jnp.int32, (HD // 2, TOK), 0).astype(F32) * 2.0 / HD))
    angles = pos_ref[:].astype(F32) * freq
    cosT[:] = jnp.cos(angles)
    sinT[:] = jnp.sin(angles)
    for c in start_cps:
        c.wait()
    proj_copies(0)[2].start()

    def rope(a):
        lo, hi = a[0:32], a[32:HD]
        return jnp.concatenate([lo * cosT[:] - hi * sinT[:], hi * cosT[:] + lo * sinT[:]], axis=0)

    def project(w):
        return lax.dot_general(w, h_ref[:], NT, preferred_element_type=F32).astype(BF16)

    def layer_body(layer, carry):
        kv = kv_all.at[layer]
        xf = x_ref[:].astype(F32)
        inv = lax.rsqrt(jnp.mean(xf * xf, axis=-1, keepdims=True) + EPS)
        gain = jnp.where(layer == 0, gain_ref[0:1, :].astype(F32), gain_ref[1:2, :].astype(F32))
        h_ref[:] = (xf * inv * gain).astype(BF16)

        w_cps = proj_copies(layer)
        w_cps[0].wait()
        w_cps[1].wait()
        kT = project(wkvb[:TOK])
        vT = project(wkvb[TOK:])
        for t in FOUR:
            k = rope(kT[t * HD:(t + 1) * HD].astype(F32)).astype(BF16)
            k_ref[layer, t * HD:(t + 1) * HD, :] = k
            kf = k.astype(F32)
            kv_send[layer, t, 0:LN, :] = jnp.concatenate([kf[:, :LN], kf[:, LN:TOK]], axis=0).T.astype(BF16)
            v = vT[t * HD:(t + 1) * HD]
            v_ref[layer, t * HD:(t + 1) * HD, :] = v
            kv_send[layer, t, LN:LN + HD, :] = v[:, :LN]
            kv_send[layer, t, LN + HD:TOK, :] = v[:, LN:TOK]

        @pl.when(layer == 0)
        def _():
            first_tiles(0)

        @pl.when(layer == 0)
        def _():
            pl.semaphore_wait(barrier, 12 - 2 * me.flag + 4 * (1 - me.mem[2]))

        def kv_copy(t):
            return remote(kv_send.at[layer, t], kv.at[me.seq], skv.at[layer, t], rkv.at[layer, me.member], me.target(t), me.core)

        def q_copy(t):
            return remote(q_send.at[layer, t], q_all.at[layer, me.member], sq.at[layer, t], rq.at[layer, me.member], me.target(t), me.core)

        def second_copy(t):
            return remote(kv_send.at[layer, t], kv.at[me.seq], skv.at[layer, 4 + t], rag.at[layer, me.mem[1], 0], me.second(t), me.core)

        for_others(me.t_self, lambda t: kv_copy(t).start())

        @pl.when(me.mem[2] == 0)
        def _():
            for t in FOUR:
                second_copy(t).start()
        for t in FOUR:
            @pl.when(me.t_self(t) == 1)
            def _():
                kv[me.seq] = kv_send[layer, t]

        w_cps[2].wait()
        for t in FOUR:
            qT = project(wqb[t * TOK:(t + 1) * TOK])
            for g in FOUR:
                q_send[layer, t, g * HD:(g + 1) * HD, :] = rope(qT[g * HD:(g + 1) * HD].astype(F32)).astype(BF16)

        def send_queries():
            for_others(me.t_self, lambda t: q_copy(t).start())
            for t in FOUR:
                @pl.when(me.t_self(t) == 1)
                def _():
                    q_all[layer, me.member] = q_send[layer, t]

        def ag(i, k):
            dim, crossed = SENDS[k]
            block = kv.at[me.across(i, crossed)]
            return remote(block, block, sag.at[layer], rag.at[layer, i, k], me.seq + me.steps(i, me.mem)[dim], me.head)

        def relay(i, crossed):
            block = kv.at[me.across(i, crossed)]
            remote(block, block, sdd.at[layer], rdd.at[layer, min(i, 2)], me.seq, sib).start()

        def arrived(i, k):
            dim, crossed = SENDS[k]
            block = kv.at[me.across(i, crossed + (dim,))]
            remote(block, block, sag.at[layer], rag.at[layer, i, k], me.seq, sib).wait_recv()

        def step(part, number):
            members = PARTS[part]
            if number == 0:
                for i in members:
                    @pl.when(me.s_self(i) == 0)
                    def _():
                        remote(kv_send.at[layer, 0], kv.at[me.source(i)], skv.at[layer, 0], rkv.at[layer, i], me.seq, sib).wait_recv()
                for k in ((1, 3) if part < 2 else (0, 1, 3)):
                    for i in members:
                        ag(i, k).start()
                for i in members:
                    relay(i, ())
            first = (0,) if number == (part == 2) else ()
            waits = first if number < 2 else SECOND if number == 2 else THIRD
            for k in waits:
                for i in members:
                    arrived(i, k)
                    for nxt in NEXT[k]:
                        ag(i, nxt).start()
            for k in waits:
                for i in members:
                    relay(i, SENDS[k][1] + (SENDS[k][0],))

        def from_sibling(part):
            blocks = kv.at[pl.ds(0, 8 * len(PARTS[part]))]
            remote(blocks, blocks, sdd.at[layer], rdd.at[layer, part], me.seq, sib).wait_recv()

        def gate_up(n):
            g = jnp.dot(h_ref[:], wgb[n % 3], preferred_element_type=F32)
            u = jnp.dot(h_ref[:], wub[n % 3], preferred_element_type=F32)
            return (g * jax.nn.sigmoid(g) * u).astype(BF16)

        def add_down(hidden, n):
            d = jnp.dot(hidden, wdb[n % 3], preferred_element_type=F32)
            for c in range(8):
                part = d[:, c * TOK:(c + 1) * TOK]
                mlp[layer, c] = part if n == 0 else mlp[layer, c] + part

        for c in gu_copies(layer, 0):
            c.wait()
        hid[:] = gate_up(0)
        for c in gu_copies(layer, 3):
            c.start()
        d_copy(layer, 2).start()

        def tile(n):
            for c in gu_copies(layer, n):
                c.wait()
            d_copy(layer, n - 1).wait()
            before = hid[:]
            now = gate_up(n)
            add_down(before, n - 1)
            hid[:] = now
            if n + 3 < N_TILES:
                for c in gu_copies(layer, n + 3):
                    c.start()
            if n + 2 < N_TILES:
                d_copy(layer, n + 2).start()

        for n in range(1, BEFORE):
            for part, number in EVENTS.get(n, ()):
                step(part, number)
            if n == 4:
                send_queries()
            tile(n)

        o_cp = pltpu.make_async_copy(wo.at[layer], wob, osem.at[0])
        o_cp.start()

        @pl.when(layer == 0)
        def _():
            for c in proj_copies(1):
                c.start()
        for part, number in EVENTS[BEFORE]:
            step(part, number)
        for_others(me.s_self, lambda i: remote(q_send.at[layer, 0], q_all.at[layer, i], sq.at[layer, 0], rq.at[layer, i], me.seq, sib).wait_recv())
        from_sibling(0)

        def o_copy(i):
            return remote(o_send.at[layer, i], o_full.at[layer, me.kv_local], so.at[layer, i], ro.at[layer, me.kv_local], me.source(i), me.mem[2])

        lax.fori_loop(0, 4, lambda i, carry: attn_start(i, q_all[layer, i], state) or carry, 0)
        def early(n, carry):
            attn_early(n, kv, state)
            for e in FOUR:
                @pl.when(n == e)
                def _():
                    for which, number in EVENTS[N_TILES + e]:
                        step(which, number)
                    if e == 1:
                        from_sibling(1)
            return carry

        lax.fori_loop(0, 4, early, 0)

        def query(i, carry):
            @pl.when(i == 2)
            def _():
                from_sibling(2)

            o_send[layer, i] = attn_block(i, me.source(i), kv, state)

            @pl.when(i == 0)
            def _():
                for part, number in EVENTS[N_TILES + 4]:
                    step(part, number)

            @pl.when(me.s_self(i) == 0)
            def _():
                o_copy(i).start()

            @pl.when(me.s_self(i) == 1)
            def _():
                o_full[layer, me.kv_local] = o_send[layer, i]
            return carry

        lax.fori_loop(0, 4, query, 0)
        for n in range(BEFORE, N_TILES):
            tile(n)
        d_copy(layer, N_TILES - 1).wait()
        add_down(hid[:], N_TILES - 1)

        @pl.when(layer == 0)
        def _():
            first_tiles(1)

        o_cp.wait()
        for_others(me.t_self, lambda t: remote(o_send.at[layer, 0], o_full.at[layer, t], so.at[layer, 0], ro.at[layer, t], me.seq, sib).wait_recv())

        def p_copy(n):
            return remote(mlp.at[layer, n], part_in.at[layer, n], sp.at[layer], rp.at[layer, n], me.seq, sib)

        heads = jnp.concatenate([o_full[layer, t] for t in FOUR], axis=1)
        for n in range(0, 8, 2):
            d = jnp.dot(heads, wob[:, n * TOK:(n + 2) * TOK], preferred_element_type=F32)
            for e in range(2):
                mlp[layer, n + e] += d[:, e * TOK:(e + 1) * TOK]
                p_copy(n + e).start()
        for n in range(8):
            cols = pl.ds(n * TOK, TOK)
            p_copy(n).wait_recv()
            y = (mlp[layer, n] + part_in[layer, n]).astype(BF16)
            x_ref[:, cols] = (x_ref[:, cols].astype(F32) + y.astype(F32)).astype(BF16)
        return carry

    lax.fori_loop(0, 2, layer_body, 0)

    def drain(layer, carry):
        def gone(src, sem):
            remote(src, src, sem, rp.at[layer, 0], me.seq, sib).wait_send()

        for_others(me.t_self, lambda t: gone(kv_send.at[layer, t], skv.at[layer, t]))
        for_others(me.t_self, lambda t: gone(q_send.at[layer, t], sq.at[layer, t]))
        for_others(me.s_self, lambda i: gone(o_send.at[layer, i], so.at[layer, i]))
        gone(kv_all.at[layer, pl.ds(0, 26)], sag.at[layer])

        @pl.when(me.mem[2] == 0)
        def _():
            for t in FOUR:
                gone(kv_send.at[layer, t], skv.at[layer, 4 + t])
        gone(kv_all.at[layer, pl.ds(0, 32)], sdd.at[layer])
        gone(mlp.at[layer], sp.at[layer])
        return carry

    lax.fori_loop(0, 2, drain, 0)


def finish_kernel(x_in, k_in, v_in, x_out, k_out, v_out, sem):
    cps = [pltpu.make_async_copy(a, b, sem.at[n]) for n, (a, b) in enumerate(((x_in, x_out), (k_in, k_out), (v_in, v_out)))]
    for c in cps:
        c.start()
    for c in cps:
        c.wait()


def vmem(*shape, dtype=BF16):
    return pltpu.VMEM(shape, dtype)


BEFORE = 15
EVENTS = {5: ((0, 0),), 7: ((1, 0),), 9: ((0, 2),), 11: ((1, 2),), 12: ((2, 0),), 13: ((0, 4),), 15: (), 16: ((1, 4), (2, 1)), 17: (), 18: ((2, 2),), 19: (), 20: ((2, 4),)}


SCRATCH = [
    vmem(32, TOK, dtype=F32), vmem(32, TOK, dtype=F32), vmem(TOK, DM), vmem(2, 4, TOK, TOK), vmem(2, 4, TOK, LN), vmem(2, 4, TOK, TOK), vmem(2, HD, TOK, LN),
    vmem(2, 4, TOK, TOK), vmem(2, 4, TOK, TOK), vmem(2, 8, TOK, TOK, dtype=F32), vmem(2, 8, TOK, TOK, dtype=F32), vmem(TOK, TOK),
    vmem(QW, DM), vmem(2 * TOK, DM), vmem(3, DM, TOK), vmem(3, DM, TOK), vmem(3, TOK, DM), vmem(QW, DM),
    vmem(4, LN, QW), vmem(4, LN, QW), vmem(4, 8, QW, dtype=F32), vmem(4, RC, QW, dtype=F32), vmem(4, HD, QW, dtype=F32), vmem(2 * TK, QW, dtype=F32), vmem(2 * RC, QW, dtype=F32),
] + [pltpu.SemaphoreType.DMA(s) for s in ((1,), (3,), (3, 3), (1,), (2, 8), (2, 4), (2,), (2,), (2, 4), (2,), (2, 4), (2, 4), (2, 4, 7), (2, 3), (2, 4), (2, 8))]


def solution(mesh):
    row_spec = P(('batch', 'seq'), None)
    pos_spec = P(('batch', 'seq'))
    head_spec = P(None, None, 'head', None)
    out_proj_spec = P(None, 'head', None, None)
    col_spec = P(None, None, 'head')
    down_spec = P(None, 'head', None)
    cache_spec = P(None, ('batch', 'seq'), 'head', None)
    in_vmem = pl.BlockSpec(memory_space=pltpu.VMEM)
    anywhere = pl.BlockSpec(memory_space=pl.ANY)

    def local_forward(x, pos, w_q, w_k, w_v, w_o, w_gate, w_up, w_down, gain):
        wq = w_q.transpose(0, 2, 3, 1).reshape(2, QW, DM)
        wk = w_k.transpose(0, 2, 3, 1).reshape(2, TOK, DM)
        wv = w_v.transpose(0, 2, 3, 1).reshape(2, TOK, DM)
        wo = w_o.reshape(2, QW, DM)
        x, kT, vT = pl.pallas_call(
            stack_kernel,
            out_shape=tuple(pltpu.VMEM(s, BF16) for s in OUT_SHAPES),
            in_specs=[anywhere] + [in_vmem] * 2 + [anywhere] * 7,
            out_specs=(in_vmem,) * 3,
            scratch_shapes=SCRATCH,
            compiler_params=pltpu.CompilerParams(collective_id=0, has_side_effects=True, vmem_limit_bytes=VMEM_LIMIT),
            name='stack',
        )(x, gain, pos.reshape(1, TOK), wq, wk, wv, w_gate, w_up, w_down, wo)
        x, kT, vT = pl.pallas_call(
            finish_kernel,
            out_shape=tuple(jax.ShapeDtypeStruct(s, BF16) for s in OUT_SHAPES),
            in_specs=[in_vmem] * 3,
            out_specs=(anywhere,) * 3,
            scratch_shapes=[pltpu.SemaphoreType.DMA((3,))],
            compiler_params=pltpu.CompilerParams(vmem_limit_bytes=QW * QW),
            name='finish',
        )(*[pltpu.with_memory_space_constraint(a, pltpu.VMEM) for a in (x, kT, vT)])
        k_cache = kT.reshape(2, 4, HD, TOK).transpose(0, 3, 1, 2)
        v_cache = vT.reshape(2, 4, HD, TOK).transpose(0, 3, 1, 2)
        return x, k_cache, v_cache

    return jax.shard_map(local_forward, mesh=mesh, in_specs=(row_spec, pos_spec, head_spec, head_spec, head_spec, out_proj_spec, col_spec, col_spec, down_spec, P(None, None)), out_specs=(row_spec, cache_spec, cache_spec), check_vma=False)


OUT_SHAPES = ((TOK, DM), (2, TOK, TOK), (2, TOK, TOK))
```
